128 devices in a mesh: zone: 4 (over y), tile: 32 (over x, z, core).
Axes of the slice: x: 4, y: 4, z: 4, core: 2. Of those that a mesh axis runs over, the one named last changes fastest.
Arguments:
- tiles: bfloat16 [384, 13, 256, 256], P(('zone', 'tile')), may hold values from -6 to 6
- seam_list: int32 [256], P(('zone', 'tile')), may hold values from 0 to 2, as said below
- source: int32 [3072], P('zone'), may hold values from 0 to 95, as said below
- offsets: int32 [3072, 2], P('zone'), may hold values from -2 to 2
- fractions: float32 [3072, 2], P('zone'), may hold values from 0 to 1
- blend: float32 [3072], P('zone'), may hold values from 0.25 to 0.75
Outputs:
- polar_blocks: bfloat16 [3072, 13, 128, 128], P(('zone', 'tile'))
The draws below stay inside these ranges and needn't reach their ends.
Inputs may be any that keep to these rules, and one draw needn't show every extreme that they name: Within the blocks of one owner device, no source device (index v // 3 of the strip) supplies more than 2 blocks; in every draw each owner takes exactly 2 blocks from some source device. Source devices are unevenly popular. `seam_list`: the 2 entries of one device are distinct.
All inputs are finite; a program needn't handle non-finite values.
Results may differ from the reference program's by a relative error of at most 0.0062.
Values may be sent and summed in bfloat16 or wider, within the bound.
No kernel may reach another device: no remote copies, remote signals or barrier semaphores. Data moves between devices by JAX's collectives and lax.ppermute only.
A program may use at most 192 MiB of HBM per device.

```python
import jax
import jax.numpy as jnp
from jax import lax

BANDS = 13
TR = 256
TC = 256
LOC = 3
OB = 24
SEAM_MAX = 2
CAP = 2
TILES = 384
BLOCKS = 3072
N_ZONE = 4
N_TILE = 32
DEVICES = 128


def draw_seam_list(key, part):
    keys = jax.random.split(key, DEVICES)

    def pick(device_key):
        return jax.random.permutation(device_key, LOC)[:SEAM_MAX].astype(jnp.int32)
    return jax.vmap(pick)(keys).reshape(DEVICES * SEAM_MAX)


def draw_source(key, part):
    entries = N_TILE * CAP
    popular = jax.random.randint(jax.random.fold_in(key, 11), (N_ZONE, N_TILE), 0, 4)
    owner_keys = jax.random.split(jax.random.fold_in(key, 23), DEVICES)

    def owner(owner_key, owner_index):
        first_key, score_key, order_key, tile_key = jax.random.split(owner_key, 4)
        entry_ids = jnp.arange(entries, dtype=jnp.int32)
        entry_device = entry_ids // CAP
        favourite = jax.random.randint(first_key, (), 0, N_TILE)
        level = popular[owner_index // N_TILE][entry_device]
        score = jax.random.randint(score_key, (entries,), 0, 1024) + 1024 * level
        score = jnp.where(entry_device == favourite, -1, score)
        ranked = jnp.argsort(score * entries + entry_ids, stable=True)[:OB]
        chosen = entry_device[ranked]
        chosen = chosen[jax.random.permutation(order_key, OB)]
        local_tile = jax.random.randint(tile_key, (OB,), 0, LOC)
        return (chosen * LOC + local_tile).astype(jnp.int32)
    return jax.vmap(owner)(owner_keys, jnp.arange(DEVICES, dtype=jnp.int32)).reshape(DEVICES * OB)


def with_ends(array, stream_key, least, top_value):
    longest = array.shape.index(max(array.shape))
    spots = []
    for shift in (0, 1):
        where = [jax.random.randint(jax.random.fold_in(stream_key, axis), (), 0, length) for axis, length in enumerate(array.shape)]
        where[longest] = (where[longest] + shift) % array.shape[longest]
        spots.append(tuple(where))
    return array.at[spots[0]].set(least).at[spots[1]].set(top_value)


def steps_of(own_key, shape, shards, least, high):
    def one(position, parts):
        draws = jax.random.uniform(jax.random.fold_in(jax.random.fold_in(own_key, 6), position), (parts,), jnp.float32, least / len(shards), high / len(shards))
        return jnp.repeat(jnp.exp(draws), shape[position] // parts).reshape((-1,) + (1,) * (len(shape) - position - 1))

    gain = one(*shards[0])
    for cut in shards[1:]:
        gain = gain * one(*cut)
    return gain


def noise(rng, dims, scale, reach, shards=(), kind=jnp.bfloat16):
    factor_of = steps_of(rng, dims, shards, -0.22, 0.18) if shards else 1.0
    array = jax.random.normal(rng, dims, jnp.float32) * scale * factor_of
    return jnp.minimum(jnp.maximum(array, -reach), reach).astype(kind)


def setup_inputs(seed: int = 0) -> dict:
    streams_of = jax.random.split(jax.random.key(seed), 7)
    return {
        "tiles": noise(streams_of[0], (TILES, BANDS, TR, TC), 1.0, 6.0, ((0, 128),)),
        "seam_list": draw_seam_list(jax.random.fold_in(streams_of[6], 71), 0),
        "source": draw_source(jax.random.fold_in(streams_of[6], 71), 0),
        "offsets": with_ends(jax.random.randint(streams_of[3], (BLOCKS, 2), -2, 3), jax.random.fold_in(streams_of[3], 1), -2, 2).astype(jnp.int32),
        "fractions": jnp.clip(1.0 * jax.random.uniform(streams_of[4], (BLOCKS, 2), jnp.float32) ** steps_of(streams_of[4], (BLOCKS, 2), ((0, 4),), -0.2, 0.2), 0.0, 1.0),
        "blend": jnp.clip(0.25 + 0.5 * jax.random.uniform(streams_of[5], (BLOCKS,), jnp.float32) ** steps_of(streams_of[5], (BLOCKS,), ((0, 4),), -0.2, 0.2), 0.25, 0.75),
    }


def cubic_weight(dist):
    mag = jnp.abs(dist)
    near = (1.5 * mag - 2.5) * mag * mag + 1.0
    far = ((-0.5 * mag + 2.5) * mag - 4.0) * mag + 2.0
    return jnp.where(mag <= 1.0, near, jnp.where(mag < 2.0, far, jnp.zeros_like(mag)))


def kernel_matrix(out_len, in_len, shift):
    rows = jnp.arange(out_len, dtype=jnp.float32)[:, None]
    cols = jnp.arange(in_len, dtype=jnp.float32)[None, :]
    return cubic_weight(cols - (2.0 * rows + shift)).astype(jnp.bfloat16)


def resample(mixed, offset_pair, fraction_pair):
    height = mixed.shape[1]
    width = mixed.shape[2]
    row_kernel = kernel_matrix(height // 2, height, offset_pair[0].astype(jnp.float32) + fraction_pair[0])
    col_kernel = kernel_matrix(width // 2, width, offset_pair[1].astype(jnp.float32) + fraction_pair[1])
    across = jnp.einsum("bkt,ot->bko", mixed.astype(jnp.float32), col_kernel.astype(jnp.float32)).astype(jnp.bfloat16)
    result = jnp.einsum("ik,bko->bio", row_kernel.astype(jnp.float32), across.astype(jnp.float32))
    return result.astype(jnp.bfloat16)


def reference(tiles, seam_list, source, offsets, fractions, blend):
    row_tiles = N_TILE * LOC
    seams = seam_list.reshape(N_ZONE * N_TILE, SEAM_MAX)

    def single(index):
        zone_index = index // (N_TILE * OB)
        value = source[index]
        primary = tiles[zone_index * row_tiles + value]
        left_zone = jnp.maximum(zone_index - 1, 0)
        secondary = tiles[left_zone * row_tiles + value]
        listed = seams[left_zone * N_TILE + value // LOC]
        flagged = jnp.any(listed == value % LOC) & (zone_index > 0)
        weight = blend[index] * flagged.astype(jnp.float32)
        mixed = ((1.0 - weight) * primary.astype(jnp.float32) + weight * secondary.astype(jnp.float32)).astype(jnp.bfloat16)
        return resample(mixed, offsets[index], fractions[index])

    return lax.map(single, jnp.arange(BLOCKS, dtype=jnp.int32), batch_size=16)
```

```python
import functools

import jax
import jax.numpy as jnp
from jax import lax
from jax.experimental import pallas as pl
from jax.experimental.pallas import tpu as pltpu
from jax.sharding import PartitionSpec as P

CHUNKS = (1, 2, 3, 4, 3)


def passed_along(value, axis, steps):
    count = lax.axis_size(axis)
    initial, last = (max(0, -steps), min(count, count - steps))
    return lax.ppermute(value, axis, [(source, source + steps) for source in range(initial, last)])


def cubic_weight(dist):
    mag = jnp.abs(dist)
    near = (1.5 * mag - 2.5) * mag * mag + 1.0
    far = ((-0.5 * mag + 2.5) * mag - 4.0) * mag + 2.0
    return jnp.where(mag <= 1.0, near, jnp.where(mag < 2.0, far, jnp.zeros_like(mag)))


def render_kernel(
    local_count, first, bands, count_ref, blocks_ref, slots_ref, source_ref, offsets_ref, fractions_ref, blend_ref,
    listed_ref, tiles_ref, near_ref, out_ref, held, beside, done, in_sem, out_sem,
):
    load = pltpu.make_async_copy(tiles_ref.at[:, pl.ds(first, bands)], held, in_sem.at[0])
    load_near = pltpu.make_async_copy(near_ref, beside, in_sem.at[1])
    load.start()
    load_near.start()
    load.wait()
    load_near.wait()
    height, width = held.shape[2], held.shape[3]
    count = count_ref[0]

    def store(index, way):
        return pltpu.make_async_copy(done.at[way], out_ref.at[slots_ref[index]], out_sem.at[way])

    def taps(shape, out_dim, shift):
        out_pos = lax.broadcasted_iota(jnp.int32, shape, out_dim).astype(jnp.float32)
        in_pos = lax.broadcasted_iota(jnp.int32, shape, 1 - out_dim).astype(jnp.float32)
        return cubic_weight(in_pos - (2.0 * out_pos + shift)).astype(jnp.bfloat16)

    def one(index, carry):
        way = lax.rem(index, 2)
        block = blocks_ref[index]
        tile = lax.rem(source_ref[block], local_count)
        second = listed_ref[1] == tile
        flagged = (second | (listed_ref[0] == tile)) & (listed_ref[2] > 0)
        place = jnp.where(second, 1, 0)
        weight = jnp.where(flagged, blend_ref[block], 0.0)
        row_kernel = taps(
            (height // 2, height), 0, offsets_ref[2 * block].astype(jnp.float32) + fractions_ref[2 * block]
        )
        col_kernel = taps(
            (width, width // 2), 1, offsets_ref[2 * block + 1].astype(jnp.float32) + fractions_ref[2 * block + 1]
        )

        @pl.when(index >= 2)
        def _():
            store(index - 2, way).wait()

        def resample(mixed, band):
            across = jnp.dot(mixed, col_kernel, preferred_element_type=jnp.float32).astype(jnp.bfloat16)
            result = jnp.dot(row_kernel, across, preferred_element_type=jnp.float32)
            done[way, band] = result.astype(jnp.bfloat16)

        @pl.when(weight == 0.0)
        def _():
            for band in range(bands):
                resample(held[tile, band], band)

        @pl.when(weight != 0.0)
        def _():
            for band in range(bands):
                mixed = (1.0 - weight) * held[tile, band].astype(jnp.float32) + weight * beside[
                    place, band
                ].astype(jnp.float32)
                resample(mixed.astype(jnp.bfloat16), band)

        store(index, way).start()
        return carry

    lax.fori_loop(0, count, one, 0)

    @pl.when(count >= 2)
    def _():
        store(count - 2, lax.rem(count, 2)).wait()

    @pl.when(count >= 1)
    def _():
        store(count - 1, lax.rem(count + 1, 2)).wait()


def render(scalars, tiles, near, first, bands, slots):
    local_count, _, height, width = tiles.shape
    block = (bands, height // 2, width // 2)
    flops = 24 * bands * (2 * height * width * width // 2 + height * width * height // 2)
    return pl.pallas_call(
        functools.partial(render_kernel, local_count, first, bands),
        out_shape=jax.ShapeDtypeStruct((slots,) + block, jnp.bfloat16),
        in_specs=[pl.BlockSpec(memory_space=pltpu.SMEM)] * len(scalars) + [pl.BlockSpec(memory_space=pl.ANY)] * 2,
        out_specs=pl.BlockSpec(memory_space=pl.ANY),
        scratch_shapes=[
            pltpu.VMEM((local_count, bands, height, width), jnp.bfloat16),
            pltpu.VMEM((near.shape[0], bands, height, width), jnp.bfloat16),
            pltpu.VMEM((2,) + block, jnp.bfloat16),
            pltpu.SemaphoreType.DMA((2,)),
            pltpu.SemaphoreType.DMA((2,)),
        ],
        cost_estimate=pl.CostEstimate(flops=8 * flops, bytes_accessed=24 * bands * height * width // 2, transcendentals=0),
        name="render",
    )(*scalars, tiles, near)


def place_kernel(first, bands, pick_ref, incoming_ref, *refs):
    out_ref, held, in_sem, out_sem = refs[-4:]
    count = out_ref.shape[0]

    def take(index):
        return pltpu.make_async_copy(incoming_ref.at[pick_ref[index]], held.at[index], in_sem.at[index])

    def put(index):
        return pltpu.make_async_copy(held.at[index], out_ref.at[index, pl.ds(first, bands)], out_sem.at[index])

    for index in range(count):
        take(index).start()
    for index in range(count):
        take(index).wait()
        put(index).start()
    for index in range(count):
        put(index).wait()


def place(pick, incoming, output, first, shape):
    bands = incoming.shape[1]
    held = (shape[0], bands) + shape[2:]
    arrays = [incoming] + ([] if output is None else [output])
    return pl.pallas_call(
        functools.partial(place_kernel, first, bands),
        out_shape=jax.ShapeDtypeStruct(shape, jnp.bfloat16),
        in_specs=[pl.BlockSpec(memory_space=pltpu.SMEM)] + [pl.BlockSpec(memory_space=pl.ANY)] * len(arrays),
        out_specs=pl.BlockSpec(memory_space=pl.ANY),
        scratch_shapes=[
            pltpu.VMEM(held, jnp.bfloat16),
            pltpu.SemaphoreType.DMA((shape[0],)),
            pltpu.SemaphoreType.DMA((shape[0],)),
        ],
        input_output_aliases={} if output is None else {2: 0},
        cost_estimate=pl.CostEstimate(flops=0, bytes_accessed=4 * shape[0] * bands * shape[2] * shape[3], transcendentals=0),
        name="place",
    )(pick, *arrays)


def local(tiles, seam_list, source, offsets, fractions, blend):
    tile_count = lax.axis_size("tile")
    myself = lax.axis_index("tile")
    zone_index = lax.axis_index("zone")
    local_count, band_count, height, width = tiles.shape
    per_owner = source.shape[0] // tile_count
    capacity = max(2, 2 * per_owner // tile_count)
    slots = tile_count * capacity

    near_list = passed_along(seam_list, "zone", 1)
    listed = jnp.concatenate([near_list, zone_index[None].astype(jnp.int32)])

    src_device = (source // local_count).reshape(tile_count, per_owner)
    order_ids = jnp.arange(per_owner, dtype=jnp.int32)
    owner_ids = jnp.arange(tile_count, dtype=jnp.int32)
    mine = src_device == myself
    earlier = order_ids[None, :] < order_ids[:, None]
    rank = jnp.sum((mine[:, None, :] & earlier[None]).astype(jnp.int32), axis=2)
    held_by = jnp.sum(mine.astype(jnp.int32), axis=1)
    ahead = jnp.sum(jnp.where(owner_ids[None, :] < owner_ids[:, None], held_by[None, :], 0), axis=1)
    turn = jnp.where(mine, rank + ahead[:, None], -1)
    hit = turn[None] == jnp.arange(slots, dtype=jnp.int32)[:, None, None]
    block_ids = owner_ids[:, None] * per_owner + order_ids[None, :]
    slot_ids = owner_ids[:, None] * capacity + rank
    blocks = jnp.sum(jnp.where(hit, block_ids[None], 0), axis=(1, 2))
    into = jnp.sum(jnp.where(hit, slot_ids[None], 0), axis=(1, 2))
    count = jnp.sum(held_by)[None]

    own = lax.dynamic_index_in_dim(src_device, myself, 0, keepdims=False)
    own_rank = jnp.sum(((own[:, None] == own[None, :]) & earlier).astype(jnp.int32), axis=1)
    pick = own * capacity + own_rank

    scalars = (count, blocks, into, source, offsets.reshape(-1), fractions.reshape(-1), blend, listed)
    shape = (per_owner, band_count, height // 2, width // 2)
    output = None
    first = 0
    for bands in CHUNKS:
        part = tiles[:, first : first + bands]
        picked = jnp.concatenate(
            [lax.dynamic_index_in_dim(part, seam_list[i], 0) for i in range(seam_list.shape[0])], axis=0
        )
        near = passed_along(picked, "zone", 1)
        outgoing = render(scalars, tiles, near, first, bands, slots)
        incoming = lax.all_to_all(
            outgoing.reshape((tile_count, capacity) + outgoing.shape[1:]), "tile", split_axis=0, concat_axis=0, tiled=True
        )
        output = place(pick, incoming.reshape((slots,) + outgoing.shape[1:]), output, first, shape)
        first += bands
    return output


def solution(mesh):
    in_specs = (
        P(("zone", "tile"), None, None, None),
        P(("zone", "tile")),
        P("zone"),
        P("zone", None),
        P("zone", None),
        P("zone"),
    )
    out_specs = P(("zone", "tile"), None, None, None)
    return jax.shard_map(local, mesh=mesh, in_specs=in_specs, out_specs=out_specs, check_vma=False)
```

```python
import functools

import jax
import jax.numpy as jnp
from jax import lax
from jax.experimental import pallas as pl
from jax.experimental.pallas import tpu as pltpu
from jax.sharding import PartitionSpec as P


CHUNKS = (2, 4, 7)
ABREAST = 4
STEPS = (-1, 0, 1, 2)


def passed_along(value, axis, steps):
    count = lax.axis_size(axis)
    initial, last = (max(0, -steps), min(count, count - steps))
    return lax.ppermute(value, axis, [(source, source + steps) for source in range(initial, last)])


def cubic_weight(dist):
    mag = jnp.abs(dist)
    near = (1.5 * mag - 2.5) * mag * mag + 1.0
    far = ((-0.5 * mag + 2.5) * mag - 4.0) * mag + 2.0
    return jnp.where(mag <= 1.0, near, jnp.where(mag < 2.0, far, jnp.zeros_like(mag)))


def render_kernel(
    local_count, first, bands, count_ref, blocks_ref, slots_ref, source_ref, offsets_ref, taps_ref, blend_ref,
    listed_ref, tiles_ref, near_ref, out_ref, held, beside, row_lag, col_lag, done, in_sem, out_sem,
):
    load = pltpu.make_async_copy(tiles_ref.at[:, pl.ds(first, bands)], held, in_sem.at[0])
    load_near = pltpu.make_async_copy(near_ref, beside, in_sem.at[1])
    load.start()
    load_near.start()
    height, width = held.shape[2], held.shape[3]
    row_lag[...] = lax.broadcasted_iota(jnp.int32, row_lag.shape, 1) - 2 * lax.broadcasted_iota(jnp.int32, row_lag.shape, 0)
    col_lag[...] = lax.broadcasted_iota(jnp.int32, col_lag.shape, 0) - 2 * lax.broadcasted_iota(jnp.int32, col_lag.shape, 1)
    load.wait()
    load_near.wait()
    count = count_ref[0]

    def store(index):
        way = lax.rem(index, 2 * ABREAST)
        return pltpu.make_async_copy(done.at[way], out_ref.at[slots_ref[index]], out_sem.at[way])

    def kernel_matrix(lag_ref, block, axis):
        lag = lag_ref[...] - offsets_ref[2 * block + axis]
        kernel = jnp.zeros(lag.shape, jnp.float32)
        for place, step in enumerate(STEPS):
            kernel = jnp.where(lag == step, taps_ref[(len(STEPS) * axis + place) * source_ref.shape[0] + block], kernel)
        return kernel.astype(jnp.bfloat16)

    def render_one(index):
        block = blocks_ref[index]
        tile = lax.rem(source_ref[block], local_count)
        second = listed_ref[1] == tile
        flagged = (second | (listed_ref[0] == tile)) & (listed_ref[2] > 0)
        place = jnp.where(second, 1, 0)
        weight = jnp.where(flagged, blend_ref[block], 0.0)
        row_kernel = kernel_matrix(row_lag, block, 0)
        col_kernel = kernel_matrix(col_lag, block, 1)
        mixed = (1.0 - weight) * held[tile].astype(jnp.float32) + weight * beside[place].astype(jnp.float32)
        mixed = mixed.astype(jnp.bfloat16).reshape(bands * height, width)
        across = jnp.dot(mixed, col_kernel, preferred_element_type=jnp.float32).astype(jnp.bfloat16)
        beside_each = jnp.concatenate([across[b * height : (b + 1) * height] for b in range(bands)], axis=1)
        return jnp.dot(row_kernel, beside_each, preferred_element_type=jnp.float32).astype(jnp.bfloat16)

    def some(turn, carry):
        start = turn * ABREAST
        for ahead in range(ABREAST):
            @pl.when(turn >= 2)
            def _():
                store(start + ahead - 2 * ABREAST).wait()
        results = [render_one(jnp.minimum(start + ahead, count - 1)) for ahead in range(ABREAST)]
        for ahead in range(ABREAST):
            way = lax.rem(start + ahead, 2 * ABREAST)
            for b in range(bands):
                done[way, b] = results[ahead][:, b * (width // 2) : (b + 1) * (width // 2)]
        for ahead in range(ABREAST):
            @pl.when(start + ahead < count)
            def _():
                store(start + ahead).start()
        return carry

    turns = lax.div(count + ABREAST - 1, ABREAST)
    lax.fori_loop(0, turns, some, 0)

    def drain(index, carry):
        store(index).wait()
        return carry

    lax.fori_loop(jnp.maximum(turns - 2, 0) * ABREAST, count, drain, 0)


def render(scalars, tiles, near, first, bands, slots):
    local_count, _, height, width = tiles.shape
    block = (bands, height // 2, width // 2)
    flops = 24 * bands * (2 * height * width * width // 2 + height * width * height // 2)
    return pl.pallas_call(
        functools.partial(render_kernel, local_count, first, bands),
        out_shape=jax.ShapeDtypeStruct((slots,) + block, jnp.bfloat16),
        in_specs=[pl.BlockSpec(memory_space=pltpu.SMEM)] * len(scalars) + [pl.BlockSpec(memory_space=pl.ANY)] * 2,
        out_specs=pl.BlockSpec(memory_space=pl.ANY),
        scratch_shapes=[
            pltpu.VMEM((local_count, bands, height, width), jnp.bfloat16),
            pltpu.VMEM((near.shape[0], bands, height, width), jnp.bfloat16),
            pltpu.VMEM((height // 2, height), jnp.int32),
            pltpu.VMEM((width, width // 2), jnp.int32),
            pltpu.VMEM((2 * ABREAST,) + block, jnp.bfloat16),
            pltpu.SemaphoreType.DMA((2,)),
            pltpu.SemaphoreType.DMA((2 * ABREAST,)),
        ],
        cost_estimate=pl.CostEstimate(flops=8 * flops, bytes_accessed=24 * bands * height * width // 2, transcendentals=0),
        name="render",
    )(*scalars, tiles, near)


def place_kernel(first, bands, pick_ref, incoming_ref, *refs):
    out_ref, held, in_sem, out_sem = refs[-4:]
    count = out_ref.shape[0]

    def take(index):
        return pltpu.make_async_copy(incoming_ref.at[pick_ref[index]], held.at[index], in_sem.at[index])

    def put(index):
        return pltpu.make_async_copy(held.at[index], out_ref.at[index, pl.ds(first, bands)], out_sem.at[index])

    for index in range(count):
        take(index).start()
    for index in range(count):
        take(index).wait()
        put(index).start()
    for index in range(count):
        put(index).wait()


def place(pick, incoming, output, first, shape):
    bands = incoming.shape[1]
    held = (shape[0], bands) + shape[2:]
    arrays = [incoming] + ([] if output is None else [output])
    return pl.pallas_call(
        functools.partial(place_kernel, first, bands),
        out_shape=jax.ShapeDtypeStruct(shape, jnp.bfloat16),
        in_specs=[pl.BlockSpec(memory_space=pltpu.SMEM)] + [pl.BlockSpec(memory_space=pl.ANY)] * len(arrays),
        out_specs=pl.BlockSpec(memory_space=pl.ANY),
        scratch_shapes=[
            pltpu.VMEM(held, jnp.bfloat16),
            pltpu.SemaphoreType.DMA((shape[0],)),
            pltpu.SemaphoreType.DMA((shape[0],)),
        ],
        input_output_aliases={} if output is None else {2: 0},
        cost_estimate=pl.CostEstimate(flops=0, bytes_accessed=4 * shape[0] * bands * shape[2] * shape[3], transcendentals=0),
        name="place",
    )(pick, *arrays)


def local(tiles, seam_list, source, offsets, fractions, blend):
    tile_count = lax.axis_size("tile")
    myself = lax.axis_index("tile")
    zone_index = lax.axis_index("zone")
    local_count, band_count, height, width = tiles.shape
    per_owner = source.shape[0] // tile_count
    capacity = max(2, 2 * per_owner // tile_count)
    slots = tile_count * capacity

    near_list = passed_along(seam_list, "zone", 1)
    listed = jnp.concatenate([near_list, zone_index[None].astype(jnp.int32)])

    src_device = (source // local_count).reshape(tile_count, per_owner)
    order_ids = jnp.arange(per_owner, dtype=jnp.int32)
    owner_ids = jnp.arange(tile_count, dtype=jnp.int32)
    mine = src_device == myself
    earlier = order_ids[None, :] < order_ids[:, None]
    rank = jnp.sum((mine[:, None, :] & earlier[None]).astype(jnp.int32), axis=2)
    held_by = jnp.sum(mine.astype(jnp.int32), axis=1)
    ahead = jnp.sum(jnp.where(owner_ids[None, :] < owner_ids[:, None], held_by[None, :], 0), axis=1)
    turn = jnp.where(mine, rank + ahead[:, None], -1)
    hit = turn[None] == jnp.arange(slots, dtype=jnp.int32)[:, None, None]
    block_ids = owner_ids[:, None] * per_owner + order_ids[None, :]
    slot_ids = owner_ids[:, None] * capacity + rank
    blocks = jnp.sum(jnp.where(hit, block_ids[None], 0), axis=(1, 2))
    into = jnp.sum(jnp.where(hit, slot_ids[None], 0), axis=(1, 2))
    count = jnp.sum(held_by)[None]

    own = lax.dynamic_index_in_dim(src_device, myself, 0, keepdims=False)
    own_rank = jnp.sum(((own[:, None] == own[None, :]) & earlier).astype(jnp.int32), axis=1)
    pick = own * capacity + own_rank

    taps = jnp.concatenate([cubic_weight(step - fractions[:, axis]) for axis in range(2) for step in STEPS])
    scalars = (count, blocks, into, source, offsets.reshape(-1), taps, blend, listed)
    shape = (per_owner, band_count, height // 2, width // 2)
    starts = [sum(CHUNKS[:part]) for part in range(len(CHUNKS))]
    nears = []
    for first, bands in zip(starts, CHUNKS):
        picked = jnp.concatenate(
            [
                lax.dynamic_slice(tiles, (seam_list[i], first, 0, 0), (1, bands, height, width))
                for i in range(seam_list.shape[0])
            ],
            axis=0,
        )
        nears.append(passed_along(picked, "zone", 1))
    output = None
    for part, (first, bands) in enumerate(zip(starts, CHUNKS)):
        outgoing = render(scalars, tiles, nears[part], first, bands, slots)
        incoming = lax.all_to_all(
            outgoing.reshape((tile_count, capacity) + outgoing.shape[1:]),
            "tile",
            split_axis=0,
            concat_axis=0,
            tiled=True,
        )
        output = place(pick, incoming.reshape((slots,) + outgoing.shape[1:]), output, first, shape)
    return output


def solution(mesh):
    in_specs = (
        P(("zone", "tile"), None, None, None),
        P(("zone", "tile")),
        P("zone"),
        P("zone", None),
        P("zone", None),
        P("zone"),
    )
    out_specs = P(("zone", "tile"), None, None, None)
    return jax.shard_map(local, mesh=mesh, in_specs=in_specs, out_specs=out_specs, check_vma=False)
```

```python
import functools

import jax
import jax.numpy as jnp
from jax import lax
from jax.experimental import pallas as pl
from jax.experimental.pallas import tpu as pltpu
from jax.sharding import PartitionSpec as P


EARLY = 3
PLACE_VMEM = 16 * 1024 * 1024
ABREAST = 4
STEPS = (-1, 0, 1, 2)


def passed_along(value, axis, steps):
    count = lax.axis_size(axis)
    initial, last = (max(0, -steps), min(count, count - steps))
    return lax.ppermute(value, axis, [(source, source + steps) for source in range(initial, last)])


def cubic_weight(dist):
    mag = jnp.abs(dist)
    near = (1.5 * mag - 2.5) * mag * mag + 1.0
    far = ((-0.5 * mag + 2.5) * mag - 4.0) * mag + 2.0
    return jnp.where(mag <= 1.0, near, jnp.where(mag < 2.0, far, jnp.zeros_like(mag)))


def pick_kernel(first, bands, listed_ref, tiles_ref, picked_ref, held, in_sem, out_sem):
    count = picked_ref.shape[0]
    for index in range(count):
        pltpu.make_async_copy(
            tiles_ref.at[listed_ref[index], pl.ds(first, bands)], held.at[index], in_sem.at[index]
        ).start()
    for index in range(count):
        pltpu.make_async_copy(
            tiles_ref.at[listed_ref[index], pl.ds(first, bands)], held.at[index], in_sem.at[index]
        ).wait()
        pltpu.make_async_copy(held.at[index], picked_ref.at[index], out_sem.at[index]).start()
    for index in range(count):
        pltpu.make_async_copy(held.at[index], picked_ref.at[index], out_sem.at[index]).wait()


def pick(listed, tiles, first, bands):
    shape = (listed.shape[0], bands) + tiles.shape[2:]
    return pl.pallas_call(
        functools.partial(pick_kernel, first, bands),
        out_shape=jax.ShapeDtypeStruct(shape, tiles.dtype),
        in_specs=[pl.BlockSpec(memory_space=pltpu.SMEM), pl.BlockSpec(memory_space=pl.ANY)],
        out_specs=pl.BlockSpec(memory_space=pl.ANY),
        scratch_shapes=[
            pltpu.VMEM(shape, tiles.dtype),
            pltpu.SemaphoreType.DMA((shape[0],)),
            pltpu.SemaphoreType.DMA((shape[0],)),
        ],
        name="pick",
    )(listed, tiles)


def render_kernel(
    local_count, first, bands, seams, range_ref, blocks_ref, slots_ref, source_ref, offsets_ref, taps_ref, blend_ref,
    listed_ref, tiles_ref, *refs,
):
    if seams:
        near_ref, _, out_ref, held, beside, row_lag, col_lag, done, in_sem, out_sem = refs
        load_near = pltpu.make_async_copy(near_ref, beside, in_sem.at[1])
        load_near.start()
        start, stop = range_ref[0], range_ref[1]
    else:
        out_ref, held, row_lag, col_lag, done, in_sem, out_sem = refs
        start, stop = 0, range_ref[0]
    load = pltpu.make_async_copy(tiles_ref.at[:, pl.ds(first, bands)], held, in_sem.at[0])
    load.start()
    height, width = held.shape[2], held.shape[3]
    row_lag[...] = lax.broadcasted_iota(jnp.int32, row_lag.shape, 1) - 2 * lax.broadcasted_iota(jnp.int32, row_lag.shape, 0)
    col_lag[...] = lax.broadcasted_iota(jnp.int32, col_lag.shape, 0) - 2 * lax.broadcasted_iota(jnp.int32, col_lag.shape, 1)
    load.wait()
    if seams:
        load_near.wait()

    def store(index):
        way = lax.rem(index - start, 2 * ABREAST)
        return pltpu.make_async_copy(done.at[way], out_ref.at[slots_ref[index]], out_sem.at[way])

    def kernel_matrix(lag_ref, block, axis):
        lag = lag_ref[...] - offsets_ref[2 * block + axis]
        kernel = jnp.zeros(lag.shape, jnp.float32)
        for place, step in enumerate(STEPS):
            kernel = jnp.where(lag == step, taps_ref[(len(STEPS) * axis + place) * source_ref.shape[0] + block], kernel)
        return kernel.astype(jnp.bfloat16)

    def render_one(index):
        block = blocks_ref[index]
        tile = lax.rem(source_ref[block], local_count)
        row_kernel = kernel_matrix(row_lag, block, 0)
        col_kernel = kernel_matrix(col_lag, block, 1)
        if seams:
            place = jnp.where(listed_ref[1] == tile, 1, 0)
            weight = blend_ref[block]
            mixed = (1.0 - weight) * held[tile].astype(jnp.float32) + weight * beside[place].astype(jnp.float32)
            mixed = mixed.astype(jnp.bfloat16)
        else:
            mixed = held[tile]
        mixed = mixed.reshape(bands * height, width)
        across = jnp.dot(mixed, col_kernel, preferred_element_type=jnp.float32).astype(jnp.bfloat16)
        beside_each = jnp.concatenate([across[b * height : (b + 1) * height] for b in range(bands)], axis=1)
        return jnp.dot(row_kernel, beside_each, preferred_element_type=jnp.float32).astype(jnp.bfloat16)

    def some(turn, carry):
        begin = start + turn * ABREAST
        for ahead in range(ABREAST):

            @pl.when(turn >= 2)
            def _():
                store(begin + ahead - 2 * ABREAST).wait()

        results = [render_one(jnp.minimum(begin + ahead, stop - 1)) for ahead in range(ABREAST)]
        for ahead in range(ABREAST):
            way = lax.rem(turn, 2) * ABREAST + ahead
            for b in range(bands):
                done[way, b] = results[ahead][:, b * (width // 2) : (b + 1) * (width // 2)]
        for ahead in range(ABREAST):

            @pl.when(begin + ahead < stop)
            def _():
                store(begin + ahead).start()

        return carry

    turns = lax.div(stop - start + ABREAST - 1, ABREAST)
    lax.fori_loop(0, turns, some, 0)

    def drain(index, carry):
        store(index).wait()
        return carry

    lax.fori_loop(start + jnp.maximum(turns - 2, 0) * ABREAST, stop, drain, 0)


def render(scalars, tiles, first, bands, slots, near=None, begun=None):
    local_count, _, height, width = tiles.shape
    block = (bands, height // 2, width // 2)
    seams = near is not None
    arrays = (tiles, near, begun) if seams else (tiles,)
    flops = 12 * bands * (2 * height * width * width // 2 + height * width * height // 2)
    return pl.pallas_call(
        functools.partial(render_kernel, local_count, first, bands, seams),
        out_shape=jax.ShapeDtypeStruct((slots,) + block, jnp.bfloat16),
        in_specs=[pl.BlockSpec(memory_space=pltpu.SMEM)] * len(scalars)
        + [pl.BlockSpec(memory_space=pl.ANY)] * len(arrays),
        out_specs=pl.BlockSpec(memory_space=pl.ANY),
        scratch_shapes=[pltpu.VMEM((local_count, bands, height, width), jnp.bfloat16)]
        + ([pltpu.VMEM(near.shape, jnp.bfloat16)] if seams else [])
        + [
            pltpu.VMEM((height // 2, height), jnp.int32),
            pltpu.VMEM((width, width // 2), jnp.int32),
            pltpu.VMEM((2 * ABREAST,) + block, jnp.bfloat16),
            pltpu.SemaphoreType.DMA((2,)),
            pltpu.SemaphoreType.DMA((2 * ABREAST,)),
        ],
        input_output_aliases={len(scalars) + 2: 0} if seams else {},
        cost_estimate=pl.CostEstimate(flops=8 * flops, bytes_accessed=12 * bands * height * width // 2, transcendentals=0),
        name="seams" if seams else "render",
    )(*scalars, *arrays)


def place_kernel(taken_ref, early_ref, late_ref, out_ref, held, early_sem, late_sem, out_sem):
    count = out_ref.shape[0]
    early, late = early_ref.shape[1], late_ref.shape[1]

    def take(index):
        return pltpu.make_async_copy(
            early_ref.at[taken_ref[index]], held.at[index, pl.ds(0, early)], early_sem.at[index]
        )

    def take_late(index):
        return pltpu.make_async_copy(
            late_ref.at[taken_ref[index]], held.at[index, pl.ds(early, late)], late_sem.at[index]
        )

    def put(index):
        return pltpu.make_async_copy(held.at[index], out_ref.at[index], out_sem.at[index])

    for index in range(count):
        take(index).start()
        take_late(index).start()
    for index in range(count):
        take(index).wait()
        take_late(index).wait()
        put(index).start()
    for index in range(count):
        put(index).wait()


def place(taken, early, late, count):
    shape = (count, early.shape[1] + late.shape[1]) + early.shape[2:]
    return pl.pallas_call(
        place_kernel,
        out_shape=jax.ShapeDtypeStruct(shape, jnp.bfloat16),
        in_specs=[pl.BlockSpec(memory_space=pltpu.SMEM)] + [pl.BlockSpec(memory_space=pl.ANY)] * 2,
        out_specs=pl.BlockSpec(memory_space=pl.ANY),
        scratch_shapes=[
            pltpu.VMEM(shape, jnp.bfloat16),
            pltpu.SemaphoreType.DMA((count,)),
            pltpu.SemaphoreType.DMA((count,)),
            pltpu.SemaphoreType.DMA((count,)),
        ],
        compiler_params=pltpu.CompilerParams(vmem_limit_bytes=PLACE_VMEM),
        name="place",
    )(taken, early, late)


def swap(outgoing, capacity):
    slots = outgoing.shape[0]
    pairs = outgoing.reshape((slots // capacity, capacity) + outgoing.shape[1:])
    return lax.all_to_all(pairs, "tile", split_axis=0, concat_axis=0, tiled=True).reshape(outgoing.shape)


def local(tiles, seam_list, source, offsets, fractions, blend):
    tile_count = lax.axis_size("tile")
    myself = lax.axis_index("tile")
    zone_index = lax.axis_index("zone")
    local_count, band_count, _, _ = tiles.shape
    per_owner = source.shape[0] // tile_count
    capacity = max(2, 2 * per_owner // tile_count)
    slots = tile_count * capacity

    near_early = passed_along(pick(seam_list, tiles, 0, EARLY), "zone", 1)
    near_list = passed_along(seam_list, "zone", 1)
    near_late = passed_along(pick(seam_list, tiles, EARLY, band_count - EARLY), "zone", 1)

    tile_of = (source % local_count).reshape(tile_count, per_owner)
    src_device = (source // local_count).reshape(tile_count, per_owner)
    order_ids = jnp.arange(per_owner, dtype=jnp.int32)
    owner_ids = jnp.arange(tile_count, dtype=jnp.int32)
    mine = src_device == myself
    flagged = mine & jnp.any(tile_of[:, :, None] == near_list[None, None, :], axis=2) & (zone_index > 0)
    plain = mine & ~flagged
    earlier = order_ids[None, :] < order_ids[:, None]
    owners_ahead = owner_ids[None, :] < owner_ids[:, None]

    def place_in_line(members):
        within = jnp.sum((members[:, None, :] & earlier[None]).astype(jnp.int32), axis=2)
        each = jnp.sum(members.astype(jnp.int32), axis=1)
        ahead = jnp.sum(jnp.where(owners_ahead, each[None, :], 0), axis=1)
        return within, within + ahead[:, None], jnp.sum(each)

    plain_rank, plain_turn, plain_count = place_in_line(plain)
    seam_rank, seam_turn, seam_count = place_in_line(flagged)
    turn = jnp.where(plain, plain_turn, jnp.where(flagged, plain_count + seam_turn, -1))
    hit = turn[None] == jnp.arange(slots, dtype=jnp.int32)[:, None, None]
    block_ids = owner_ids[:, None] * per_owner + order_ids[None, :]
    slot_ids = owner_ids[:, None] * capacity + plain_rank + seam_rank
    blocks = jnp.sum(jnp.where(hit, block_ids[None], 0), axis=(1, 2))
    into = jnp.sum(jnp.where(hit, slot_ids[None], 0), axis=(1, 2))
    ranges = jnp.stack([plain_count, plain_count + seam_count])

    own = lax.dynamic_index_in_dim(src_device, myself, 0, keepdims=False)
    own_rank = jnp.sum(((own[:, None] == own[None, :]) & earlier).astype(jnp.int32), axis=1)
    taken = own * capacity + own_rank

    taps = jnp.concatenate([cubic_weight(step - fractions[:, axis]) for axis in range(2) for step in STEPS])
    scalars = (ranges, blocks, into, source, offsets.reshape(-1), taps, blend, near_list)
    outgoing = render(scalars, tiles, 0, EARLY, slots)
    outgoing = render(scalars, tiles, 0, EARLY, slots, near_early, outgoing)
    early = swap(outgoing, capacity)
    outgoing = render(scalars, tiles, EARLY, band_count - EARLY, slots)
    outgoing = render(scalars, tiles, EARLY, band_count - EARLY, slots, near_late, outgoing)
    outgoing, taken = lax.optimization_barrier((outgoing, taken))
    late = swap(outgoing, capacity)
    return place(taken, early, late, per_owner)


def solution(mesh):
    in_specs = (
        P(("zone", "tile"), None, None, None),
        P(("zone", "tile")),
        P("zone"),
        P("zone", None),
        P("zone", None),
        P("zone"),
    )
    out_specs = P(("zone", "tile"), None, None, None)
    return jax.shard_map(local, mesh=mesh, in_specs=in_specs, out_specs=out_specs, check_vma=False)
```

```python
import functools

import jax
import jax.numpy as jnp
from jax import lax
from jax.experimental import pallas as pl
from jax.experimental.pallas import tpu as pltpu
from jax.sharding import PartitionSpec as P


CHUNKS = (("x", 2), ("z", 2), ("x", 5), ("z", 4))
RING = 4
LANES = 2 * RING
ABREAST = 4
STEPS = (-1, 0, 1, 2)


def passed_along(value, axis, steps):
    count = lax.axis_size(axis)
    initial, last = (max(0, -steps), min(count, count - steps))
    return lax.ppermute(value, axis, [(source, source + steps) for source in range(initial, last)])


def cubic_weight(dist):
    mag = jnp.abs(dist)
    near = (1.5 * mag - 2.5) * mag * mag + 1.0
    far = ((-0.5 * mag + 2.5) * mag - 4.0) * mag + 2.0
    return jnp.where(mag <= 1.0, near, jnp.where(mag < 2.0, far, jnp.zeros_like(mag)))


def hop(value, along, steps, cross=0):
    pairs = []
    for x in range(RING):
        for z in range(RING):
            for core in range(2):
                to_x, to_z = ((x + steps) % RING, z) if along == "x" else (x, (z + steps) % RING)
                pairs.append(((x * RING + z) * 2 + core, (to_x * RING + to_z) * 2 + (core ^ cross)))
    return lax.ppermute(value, "tile", pairs)


def pick_kernel(first, bands, listed_ref, tiles_ref, picked_ref, held, in_sem, out_sem):
    count = picked_ref.shape[0]
    for index in range(count):
        pltpu.make_async_copy(
            tiles_ref.at[listed_ref[index], pl.ds(first, bands)], held.at[index], in_sem.at[index]
        ).start()
    for index in range(count):
        pltpu.make_async_copy(
            tiles_ref.at[listed_ref[index], pl.ds(first, bands)], held.at[index], in_sem.at[index]
        ).wait()
        pltpu.make_async_copy(held.at[index], picked_ref.at[index], out_sem.at[index]).start()
    for index in range(count):
        pltpu.make_async_copy(held.at[index], picked_ref.at[index], out_sem.at[index]).wait()


def pick(listed, tiles, first, bands):
    shape = (listed.shape[0], bands) + tiles.shape[2:]
    return pl.pallas_call(
        functools.partial(pick_kernel, first, bands),
        out_shape=jax.ShapeDtypeStruct(shape, tiles.dtype),
        in_specs=[pl.BlockSpec(memory_space=pltpu.SMEM), pl.BlockSpec(memory_space=pl.ANY)],
        out_specs=pl.BlockSpec(memory_space=pl.ANY),
        scratch_shapes=[
            pltpu.VMEM(shape, tiles.dtype),
            pltpu.SemaphoreType.DMA((shape[0],)),
            pltpu.SemaphoreType.DMA((shape[0],)),
        ],
        name="pick",
    )(listed, tiles)


def render_kernel(
    local_count, first, bands, count_ref, blocks_ref, into_ref, side_ref, source_ref, offsets_ref, taps_ref, blend_ref,
    listed_ref, tiles_ref, beyond_ref, near_ref, near_beyond_ref, stay_ref, up_ref, down_ref,
    held, beside, row_lag, col_lag, done, in_sem, out_sem,
):
    seams = near_ref.shape[0]
    loads = (
        pltpu.make_async_copy(tiles_ref.at[:, pl.ds(first, bands)], held.at[pl.ds(0, local_count)], in_sem.at[0]),
        pltpu.make_async_copy(beyond_ref, held.at[pl.ds(local_count, local_count)], in_sem.at[1]),
        pltpu.make_async_copy(near_ref, beside.at[pl.ds(0, seams)], in_sem.at[2]),
        pltpu.make_async_copy(near_beyond_ref, beside.at[pl.ds(seams, seams)], in_sem.at[3]),
    )
    for load in loads:
        load.start()
    height, width = held.shape[2], held.shape[3]
    row_lag[...] = lax.broadcasted_iota(jnp.int32, row_lag.shape, 1) - 2 * lax.broadcasted_iota(jnp.int32, row_lag.shape, 0)
    col_lag[...] = lax.broadcasted_iota(jnp.int32, col_lag.shape, 0) - 2 * lax.broadcasted_iota(jnp.int32, col_lag.shape, 1)
    for load in loads:
        load.wait()
    count = count_ref[0]

    def start_store(index, way):
        into = into_ref[index]
        slot = lax.rem(into, 64)
        for number, out_ref in ((0, stay_ref), (1, up_ref), (3, down_ref)):

            @pl.when(lax.div(into, 64) == number)
            def _():
                pltpu.make_async_copy(done.at[way], out_ref.at[slot], out_sem.at[way]).start()

    def wait_store(way):
        pltpu.make_async_copy(done.at[way], stay_ref.at[0], out_sem.at[way]).wait()

    def kernel_matrix(lag_ref, block, axis):
        lag = lag_ref[...] - offsets_ref[2 * block + axis]
        kernel = jnp.zeros(lag.shape, jnp.float32)
        for place, step in enumerate(STEPS):
            kernel = jnp.where(lag == step, taps_ref[(len(STEPS) * axis + place) * source_ref.shape[0] + block], kernel)
        return kernel.astype(jnp.bfloat16)

    def render_one(index):
        block = blocks_ref[index]
        side = side_ref[index]
        tile = lax.rem(source_ref[block], local_count)
        second = listed_ref[seams * side + 1] == tile
        flagged = (second | (listed_ref[seams * side] == tile)) & (listed_ref[2 * seams] > 0)
        place = seams * side + jnp.where(second, 1, 0)
        weight = jnp.where(flagged, blend_ref[block], 0.0)
        row_kernel = kernel_matrix(row_lag, block, 0)
        col_kernel = kernel_matrix(col_lag, block, 1)
        primary = held[local_count * side + tile].astype(jnp.float32)
        mixed = (1.0 - weight) * primary + weight * beside[place].astype(jnp.float32)
        mixed = mixed.astype(jnp.bfloat16).reshape(bands * height, width)
        across = jnp.dot(mixed, col_kernel, preferred_element_type=jnp.float32).astype(jnp.bfloat16)
        beside_each = jnp.concatenate([across[b * height : (b + 1) * height] for b in range(bands)], axis=1)
        return jnp.dot(row_kernel, beside_each, preferred_element_type=jnp.float32).astype(jnp.bfloat16)

    def some(turn, carry):
        begin = turn * ABREAST
        half = lax.rem(turn, 2) * ABREAST
        for ahead in range(ABREAST):

            @pl.when(turn >= 2)
            def _():
                wait_store(half + ahead)

        results = [render_one(jnp.minimum(begin + ahead, count - 1)) for ahead in range(ABREAST)]
        for ahead in range(ABREAST):
            for b in range(bands):
                done[half + ahead, b] = results[ahead][:, b * (width // 2) : (b + 1) * (width // 2)]
        for ahead in range(ABREAST):

            @pl.when(begin + ahead < count)
            def _():
                start_store(begin + ahead, half + ahead)

        return carry

    turns = lax.div(count + ABREAST - 1, ABREAST)
    lax.fori_loop(0, turns, some, 0)

    def drain(index, carry):
        wait_store(lax.rem(index, 2 * ABREAST))
        return carry

    lax.fori_loop(jnp.maximum(turns - 2, 0) * ABREAST, count, drain, 0)


def render(scalars, tiles, beyond, near, near_beyond, first):
    local_count, _, height, width = tiles.shape
    bands = beyond.shape[1]
    block = (bands, height // 2, width // 2)
    flops = 24 * bands * (2 * height * width * width // 2 + height * width * height // 2)
    return pl.pallas_call(
        functools.partial(render_kernel, local_count, first, bands),
        out_shape=[jax.ShapeDtypeStruct((slots,) + block, jnp.bfloat16) for slots in (4 * LANES, 2 * LANES, 2 * LANES)],
        in_specs=[pl.BlockSpec(memory_space=pltpu.SMEM)] * len(scalars) + [pl.BlockSpec(memory_space=pl.ANY)] * 4,
        out_specs=[pl.BlockSpec(memory_space=pl.ANY)] * 3,
        scratch_shapes=[
            pltpu.VMEM((2 * local_count, bands, height, width), jnp.bfloat16),
            pltpu.VMEM((2 * near.shape[0], bands, height, width), jnp.bfloat16),
            pltpu.VMEM((height // 2, height), jnp.int32),
            pltpu.VMEM((width, width // 2), jnp.int32),
            pltpu.VMEM((2 * ABREAST,) + block, jnp.bfloat16),
            pltpu.SemaphoreType.DMA((4,)),
            pltpu.SemaphoreType.DMA((2 * ABREAST,)),
        ],
        cost_estimate=pl.CostEstimate(flops=8 * flops, bytes_accessed=24 * bands * height * width // 2, transcendentals=0),
        name="render",
    )(*scalars, tiles, beyond, near, near_beyond)


def pack_kernel(stay_ref, up_ref, down_ref, *refs):
    outs, (held, in_sem, out_sem) = refs[:LANES], refs[LANES:]
    copies = []
    for lane in range(LANES):
        copies += [
            pltpu.make_async_copy(stay_ref.at[pl.ds(4 * lane, 4)], held.at[lane, pl.ds(0, 4)], in_sem.at[lane, 0]),
            pltpu.make_async_copy(up_ref.at[pl.ds(2 * lane, 2)], held.at[lane, pl.ds(4, 2)], in_sem.at[lane, 1]),
            pltpu.make_async_copy(down_ref.at[pl.ds(2 * lane, 2)], held.at[lane, pl.ds(6, 2)], in_sem.at[lane, 2]),
        ]
    for copy in copies:
        copy.start()
    puts = [pltpu.make_async_copy(held.at[lane], outs[lane], out_sem.at[lane]) for lane in range(LANES)]
    for lane in range(LANES):
        for copy in copies[3 * lane : 3 * lane + 3]:
            copy.wait()
        puts[lane].start()
    for put in puts:
        put.wait()


def pack(stay, up, down):
    shape = (8,) + stay.shape[1:]
    return pl.pallas_call(
        pack_kernel,
        out_shape=[jax.ShapeDtypeStruct(shape, stay.dtype)] * LANES,
        in_specs=[pl.BlockSpec(memory_space=pl.ANY)] * 3,
        out_specs=[pl.BlockSpec(memory_space=pl.ANY)] * LANES,
        scratch_shapes=[
            pltpu.VMEM((LANES,) + shape, stay.dtype),
            pltpu.SemaphoreType.DMA((LANES, 3)),
            pltpu.SemaphoreType.DMA((LANES,)),
        ],
        name="pack",
    )(stay, up, down)


def place_kernel(parts, x_lane_ref, x_slot_ref, z_lane_ref, z_slot_ref, *refs):
    arrays, (out_ref, held, in_sem, out_sem) = refs[: LANES * len(parts)], refs[LANES * len(parts) :]
    count = out_ref.shape[0]

    def take(index, carry):
        for number, (axis, first, bands) in enumerate(parts):
            lane_ref, slot_ref = (x_lane_ref, x_slot_ref) if axis == "x" else (z_lane_ref, z_slot_ref)
            for lane in range(LANES):

                @pl.when(lane_ref[index] == lane)
                def _():
                    pltpu.make_async_copy(
                        arrays[LANES * number + lane].at[slot_ref[index]],
                        held.at[index, pl.ds(first, bands)],
                        in_sem.at[number, index],
                    ).start()

        return carry

    lax.fori_loop(0, count, take, 0)

    def put(index, carry):
        for number, (axis, first, bands) in enumerate(parts):
            pltpu.make_async_copy(
                arrays[LANES * number].at[0], held.at[index, pl.ds(first, bands)], in_sem.at[number, index]
            ).wait()
        pltpu.make_async_copy(held.at[index], out_ref.at[index], out_sem.at[index]).start()
        return carry

    lax.fori_loop(0, count, put, 0)

    def finish(index, carry):
        pltpu.make_async_copy(held.at[index], out_ref.at[index], out_sem.at[index]).wait()
        return carry

    lax.fori_loop(0, count, finish, 0)


def place(parts, taken, arrays, shape):
    return pl.pallas_call(
        functools.partial(place_kernel, parts),
        out_shape=jax.ShapeDtypeStruct(shape, jnp.bfloat16),
        in_specs=[pl.BlockSpec(memory_space=pltpu.SMEM)] * 4 + [pl.BlockSpec(memory_space=pl.ANY)] * len(arrays),
        out_specs=pl.BlockSpec(memory_space=pl.ANY),
        scratch_shapes=[
            pltpu.VMEM(shape, jnp.bfloat16),
            pltpu.SemaphoreType.DMA((len(parts), shape[0])),
            pltpu.SemaphoreType.DMA((shape[0],)),
        ],
        name="place",
    )(*taken, *arrays)


def local(tiles, seam_list, source, offsets, fractions, blend):
    tile_count = lax.axis_size("tile")
    myself = lax.axis_index("tile")
    zone_index = lax.axis_index("zone")
    local_count, band_count, height, width = tiles.shape
    per_owner = source.shape[0] // tile_count
    slots = 8 * LANES

    parts, first = [], 0
    for axis, bands in CHUNKS:
        parts.append((axis, first, bands))
        first += bands

    nears, beyonds, nears_beyond = [], [], []
    for axis, first, bands in parts:
        nears.append(passed_along(pick(seam_list, tiles, first, bands), "zone", 1))
        beyonds.append(hop(tiles[:, first : first + bands], axis, 1))
        nears_beyond.append(hop(nears[-1], axis, 1))
    near_list = passed_along(seam_list, "zone", 1)

    def coordinates(device):
        return device // (2 * RING), (device // 2) % RING, device % 2

    order_ids = jnp.arange(per_owner, dtype=jnp.int32)
    owner_ids = jnp.arange(tile_count, dtype=jnp.int32)
    src_device = (source // local_count).reshape(tile_count, per_owner)
    earlier = order_ids[None, :] < order_ids[:, None]
    owners_ahead = owner_ids[None, :] < owner_ids[:, None]
    same = src_device[:, :, None] == src_device[:, None, :]
    rank = jnp.sum((same & earlier[None]).astype(jnp.int32), axis=2)
    block_ids = owner_ids[:, None] * per_owner + order_ids[None, :]
    my_x, my_z, my_core = coordinates(myself)
    src_x, src_z, src_core = coordinates(src_device)
    own_x, own_z, own_core = coordinates(owner_ids[:, None])
    own_src = lax.dynamic_index_in_dim(src_device, myself, 0, keepdims=False)
    own_rank = jnp.sum(((own_src[:, None] == own_src[None, :]) & earlier).astype(jnp.int32), axis=1)
    from_x, from_z, from_core = coordinates(own_src)

    def lists(my_p, my_q, src_p, src_q, own_p, own_q):
        behind = (my_p - src_p) & (RING - 1)
        ahead = (own_p - my_p) & (RING - 1)
        mine = (src_core == my_core) & (src_q == my_q)
        mine = mine & (((behind == 0) & ((ahead == 0) | (ahead == 3))) | ((behind == 1) & ((ahead == 0) | (ahead == 1))))
        lane = 2 * ((own_q - my_q) & (RING - 1)) + (own_core != my_core).astype(jnp.int32)
        slot = jnp.where(ahead == 0, 4 * lane + 2 * behind + rank, 2 * lane + rank)
        within = jnp.sum((mine[:, None, :] & earlier[None]).astype(jnp.int32), axis=2)
        each = jnp.sum(mine.astype(jnp.int32), axis=1)
        turn = within + jnp.sum(jnp.where(owners_ahead, each[None, :], 0), axis=1)[:, None]
        hit = mine[None] & (turn[None] == jnp.arange(slots, dtype=jnp.int32)[:, None, None])

        def listed(values):
            return jnp.sum(jnp.where(hit, values[None], 0), axis=(1, 2))

        return jnp.sum(each)[None], listed(block_ids), listed(64 * ahead + slot), listed(behind)

    def taken(my_p, my_q, src_p, src_q):
        lane = 2 * ((my_q - src_q) & (RING - 1)) + (from_core != my_core).astype(jnp.int32)
        return lane, 2 * ((my_p - src_p) & (RING - 1)) + own_rank

    by_axis = {
        "x": lists(my_x, my_z, src_x, src_z, own_x, own_z),
        "z": lists(my_z, my_x, src_z, src_x, own_z, own_x),
    }
    picks = taken(my_x, my_z, from_x, from_z) + taken(my_z, my_x, from_z, from_x)
    taps = jnp.concatenate([cubic_weight(step - fractions[:, axis]) for axis in range(2) for step in STEPS])
    flat_offsets = offsets.reshape(-1)
    zone_flag = zone_index[None].astype(jnp.int32)
    listed_by = {axis: jnp.concatenate([near_list, hop(near_list, axis, 1), zone_flag]) for axis in ("x", "z")}

    arrays = []
    for part, (axis, first, bands) in enumerate(parts):
        scalars = by_axis[axis] + (source, flat_offsets, taps, blend, listed_by[axis])
        stay, up, down = render(scalars, tiles, beyonds[part], nears[part], nears_beyond[part], first)
        came_up, came_down = hop(up, axis, 1), hop(down, axis, -1)
        packed = pack(stay, came_up, came_down)
        other = "z" if axis == "x" else "x"
        arrays += [packed[0]] + [hop(packed[lane], other, lane // 2, lane % 2) for lane in range(1, LANES)]
    shape = (per_owner, band_count, height // 2, width // 2)
    return place(tuple(parts), picks, arrays, shape)


def solution(mesh):
    in_specs = (
        P(("zone", "tile"), None, None, None),
        P(("zone", "tile")),
        P("zone"),
        P("zone", None),
        P("zone", None),
        P("zone"),
    )
    out_specs = P(("zone", "tile"), None, None, None)
    return jax.shard_map(local, mesh=mesh, in_specs=in_specs, out_specs=out_specs, check_vma=False)
```

```python
import functools

import jax
import jax.numpy as jnp
from jax import lax
from jax.experimental import pallas as pl
from jax.experimental.pallas import tpu as pltpu
from jax.sharding import PartitionSpec as P


CHUNKS = (("x", 3), ("z", 3), ("x", 4), ("z", 3))
RING = 4
LANES = 2 * RING
ABREAST = 4
STEPS = (-1, 0, 1, 2)


def passed_along(value, axis, steps):
    count = lax.axis_size(axis)
    initial, last = (max(0, -steps), min(count, count - steps))
    return lax.ppermute(value, axis, [(source, source + steps) for source in range(initial, last)])


def cubic_weight(dist):
    mag = jnp.abs(dist)
    near = (1.5 * mag - 2.5) * mag * mag + 1.0
    far = ((-0.5 * mag + 2.5) * mag - 4.0) * mag + 2.0
    return jnp.where(mag <= 1.0, near, jnp.where(mag < 2.0, far, jnp.zeros_like(mag)))


def ring_pairs(along, steps, cross):
    pairs = []
    for x in range(RING):
        for z in range(RING):
            for core in range(2):
                to_x, to_z = ((x + steps) % RING, z) if along == "x" else (x, (z + steps) % RING)
                pairs.append(((x * RING + z) * 2 + core, (to_x * RING + to_z) * 2 + (core ^ cross)))
    return pairs


def hop(value, along, steps, cross=0):
    return lax.ppermute(value, "tile", ring_pairs(along, steps, cross))


def pick_kernel(first, bands, listed_ref, tiles_ref, picked_ref, held, in_sem, out_sem):
    count = picked_ref.shape[0]
    for index in range(count):
        pltpu.make_async_copy(
            tiles_ref.at[listed_ref[index], pl.ds(first, bands)], held.at[index], in_sem.at[index]
        ).start()
    for index in range(count):
        pltpu.make_async_copy(
            tiles_ref.at[listed_ref[index], pl.ds(first, bands)], held.at[index], in_sem.at[index]
        ).wait()
        pltpu.make_async_copy(held.at[index], picked_ref.at[index], out_sem.at[index]).start()
    for index in range(count):
        pltpu.make_async_copy(held.at[index], picked_ref.at[index], out_sem.at[index]).wait()


def pick(listed, tiles, first, bands):
    shape = (listed.shape[0], bands) + tiles.shape[2:]
    return pl.pallas_call(
        functools.partial(pick_kernel, first, bands),
        out_shape=jax.ShapeDtypeStruct(shape, tiles.dtype),
        in_specs=[pl.BlockSpec(memory_space=pltpu.SMEM), pl.BlockSpec(memory_space=pl.ANY)],
        out_specs=pl.BlockSpec(memory_space=pl.ANY),
        scratch_shapes=[
            pltpu.VMEM(shape, tiles.dtype),
            pltpu.SemaphoreType.DMA((shape[0],)),
            pltpu.SemaphoreType.DMA((shape[0],)),
        ],
        name="pick",
    )(listed, tiles)


def render_kernel(
    local_count, first, bands, count_ref, blocks_ref, into_ref, side_ref, source_ref, offsets_ref, taps_ref, blend_ref,
    listed_ref, tiles_ref, beyond_ref, near_ref, near_beyond_ref, stay_ref, up_ref, down_ref,
    held, beside, row_lag, col_lag, done, in_sem, out_sem,
):
    seams = near_ref.shape[0]
    loads = (
        pltpu.make_async_copy(tiles_ref.at[:, pl.ds(first, bands)], held.at[pl.ds(0, local_count)], in_sem.at[0]),
        pltpu.make_async_copy(beyond_ref, held.at[pl.ds(local_count, local_count)], in_sem.at[1]),
        pltpu.make_async_copy(near_ref, beside.at[pl.ds(0, seams)], in_sem.at[2]),
        pltpu.make_async_copy(near_beyond_ref, beside.at[pl.ds(seams, seams)], in_sem.at[3]),
    )
    for load in loads:
        load.start()
    height, width = held.shape[2], held.shape[3]
    row_lag[...] = lax.broadcasted_iota(jnp.int32, row_lag.shape, 1) - 2 * lax.broadcasted_iota(jnp.int32, row_lag.shape, 0)
    col_lag[...] = lax.broadcasted_iota(jnp.int32, col_lag.shape, 0) - 2 * lax.broadcasted_iota(jnp.int32, col_lag.shape, 1)
    for load in loads:
        load.wait()
    count = count_ref[0]

    def start_store(index, way):
        into = into_ref[index]
        slot = lax.rem(into, 64)
        for number, out_ref in ((0, stay_ref), (1, up_ref), (3, down_ref)):

            @pl.when(lax.div(into, 64) == number)
            def _():
                pltpu.make_async_copy(done.at[way], out_ref.at[slot], out_sem.at[way]).start()

    def wait_store(way):
        pltpu.make_async_copy(done.at[way], stay_ref.at[0], out_sem.at[way]).wait()

    def kernel_matrix(lag_ref, block, axis):
        lag = lag_ref[...] - offsets_ref[2 * block + axis]
        kernel = jnp.zeros(lag.shape, jnp.float32)
        for place, step in enumerate(STEPS):
            kernel = jnp.where(lag == step, taps_ref[(len(STEPS) * axis + place) * source_ref.shape[0] + block], kernel)
        return kernel.astype(jnp.bfloat16)

    def render_one(index):
        block = blocks_ref[index]
        side = side_ref[index]
        tile = lax.rem(source_ref[block], local_count)
        second = listed_ref[seams * side + 1] == tile
        flagged = (second | (listed_ref[seams * side] == tile)) & (listed_ref[2 * seams] > 0)
        place = seams * side + jnp.where(second, 1, 0)
        weight = jnp.where(flagged, blend_ref[block], 0.0)
        row_kernel = kernel_matrix(row_lag, block, 0)
        col_kernel = kernel_matrix(col_lag, block, 1)
        primary = held[local_count * side + tile].astype(jnp.float32)
        mixed = (1.0 - weight) * primary + weight * beside[place].astype(jnp.float32)
        mixed = mixed.astype(jnp.bfloat16).reshape(bands * height, width)
        across = jnp.dot(mixed, col_kernel, preferred_element_type=jnp.float32).astype(jnp.bfloat16)
        beside_each = jnp.concatenate([across[b * height : (b + 1) * height] for b in range(bands)], axis=1)
        return jnp.dot(row_kernel, beside_each, preferred_element_type=jnp.float32).astype(jnp.bfloat16)

    def some(turn, carry):
        begin = turn * ABREAST
        half = lax.rem(turn, 2) * ABREAST
        for ahead in range(ABREAST):

            @pl.when(turn >= 2)
            def _():
                wait_store(half + ahead)

        results = [render_one(jnp.minimum(begin + ahead, count - 1)) for ahead in range(ABREAST)]
        for ahead in range(ABREAST):
            for b in range(bands):
                done[half + ahead, b] = results[ahead][:, b * (width // 2) : (b + 1) * (width // 2)]
        for ahead in range(ABREAST):

            @pl.when(begin + ahead < count)
            def _():
                start_store(begin + ahead, half + ahead)

        return carry

    turns = lax.div(count + ABREAST - 1, ABREAST)
    lax.fori_loop(0, turns, some, 0)

    def drain(index, carry):
        wait_store(lax.rem(index, 2 * ABREAST))
        return carry

    lax.fori_loop(jnp.maximum(turns - 2, 0) * ABREAST, count, drain, 0)


def render(scalars, tiles, beyond, near, near_beyond, first):
    local_count, _, height, width = tiles.shape
    bands = beyond.shape[1]
    block = (bands, height // 2, width // 2)
    flops = 24 * bands * (2 * height * width * width // 2 + height * width * height // 2)
    return pl.pallas_call(
        functools.partial(render_kernel, local_count, first, bands),
        out_shape=[jax.ShapeDtypeStruct((slots,) + block, jnp.bfloat16) for slots in (4 * LANES, 2 * LANES, 2 * LANES)],
        in_specs=[pl.BlockSpec(memory_space=pltpu.SMEM)] * len(scalars) + [pl.BlockSpec(memory_space=pl.ANY)] * 4,
        out_specs=[pl.BlockSpec(memory_space=pl.ANY)] * 3,
        scratch_shapes=[
            pltpu.VMEM((2 * local_count, bands, height, width), jnp.bfloat16),
            pltpu.VMEM((2 * near.shape[0], bands, height, width), jnp.bfloat16),
            pltpu.VMEM((height // 2, height), jnp.int32),
            pltpu.VMEM((width, width // 2), jnp.int32),
            pltpu.VMEM((2 * ABREAST,) + block, jnp.bfloat16),
            pltpu.SemaphoreType.DMA((4,)),
            pltpu.SemaphoreType.DMA((2 * ABREAST,)),
        ],
        cost_estimate=pl.CostEstimate(flops=8 * flops, bytes_accessed=24 * bands * height * width // 2, transcendentals=0),
        name="render",
    )(*scalars, tiles, beyond, near, near_beyond)


def pack_kernel(stay_ref, up_ref, down_ref, *refs):
    outs, (held, in_sem, out_sem) = refs[:LANES], refs[LANES:]
    copies = []
    for lane in range(LANES):
        copies += [
            pltpu.make_async_copy(stay_ref.at[pl.ds(4 * lane, 4)], held.at[lane, pl.ds(0, 4)], in_sem.at[lane, 0]),
            pltpu.make_async_copy(up_ref.at[pl.ds(2 * lane, 2)], held.at[lane, pl.ds(4, 2)], in_sem.at[lane, 1]),
            pltpu.make_async_copy(down_ref.at[pl.ds(2 * lane, 2)], held.at[lane, pl.ds(6, 2)], in_sem.at[lane, 2]),
        ]
    for copy in copies:
        copy.start()
    puts = [pltpu.make_async_copy(held.at[lane], outs[lane], out_sem.at[lane]) for lane in range(LANES)]
    for lane in range(LANES):
        for copy in copies[3 * lane : 3 * lane + 3]:
            copy.wait()
        puts[lane].start()
    for put in puts:
        put.wait()


def pack(stay, up, down):
    shape = (8,) + stay.shape[1:]
    return pl.pallas_call(
        pack_kernel,
        out_shape=[jax.ShapeDtypeStruct(shape, stay.dtype)] * LANES,
        in_specs=[pl.BlockSpec(memory_space=pl.ANY)] * 3,
        out_specs=[pl.BlockSpec(memory_space=pl.ANY)] * LANES,
        scratch_shapes=[
            pltpu.VMEM((LANES,) + shape, stay.dtype),
            pltpu.SemaphoreType.DMA((LANES, 3)),
            pltpu.SemaphoreType.DMA((LANES,)),
        ],
        name="pack",
    )(stay, up, down)


def place_kernel(parts, x_lane_ref, x_slot_ref, z_lane_ref, z_slot_ref, *refs):
    arrays, (out_ref, held, in_sem, out_sem) = refs[: LANES * len(parts)], refs[LANES * len(parts) :]
    count = out_ref.shape[0]

    def take(index, carry):
        for number, (axis, first, bands) in enumerate(parts):
            lane_ref, slot_ref = (x_lane_ref, x_slot_ref) if axis == "x" else (z_lane_ref, z_slot_ref)
            for lane in range(LANES):

                @pl.when(lane_ref[index] == lane)
                def _():
                    pltpu.make_async_copy(
                        arrays[LANES * number + lane].at[slot_ref[index]],
                        held.at[index, pl.ds(first, bands)],
                        in_sem.at[number, index],
                    ).start()

        return carry

    lax.fori_loop(0, count, take, 0)

    def put(index, carry):
        for number, (axis, first, bands) in enumerate(parts):
            pltpu.make_async_copy(
                arrays[LANES * number].at[0], held.at[index, pl.ds(first, bands)], in_sem.at[number, index]
            ).wait()
        pltpu.make_async_copy(held.at[index], out_ref.at[index], out_sem.at[index]).start()
        return carry

    lax.fori_loop(0, count, put, 0)

    def finish(index, carry):
        pltpu.make_async_copy(held.at[index], out_ref.at[index], out_sem.at[index]).wait()
        return carry

    lax.fori_loop(0, count, finish, 0)


def place(parts, taken, arrays, shape):
    return pl.pallas_call(
        functools.partial(place_kernel, parts),
        out_shape=jax.ShapeDtypeStruct(shape, jnp.bfloat16),
        in_specs=[pl.BlockSpec(memory_space=pltpu.SMEM)] * 4 + [pl.BlockSpec(memory_space=pl.ANY)] * len(arrays),
        out_specs=pl.BlockSpec(memory_space=pl.ANY),
        scratch_shapes=[
            pltpu.VMEM(shape, jnp.bfloat16),
            pltpu.SemaphoreType.DMA((len(parts), shape[0])),
            pltpu.SemaphoreType.DMA((shape[0],)),
        ],
        name="place",
    )(*taken, *arrays)


def local(tiles, seam_list, source, offsets, fractions, blend):
    tile_count = lax.axis_size("tile")
    myself = lax.axis_index("tile")
    zone_index = lax.axis_index("zone")
    local_count, band_count, height, width = tiles.shape
    per_owner = source.shape[0] // tile_count
    slots = 8 * LANES

    parts, first = [], 0
    for axis, bands in CHUNKS:
        parts.append((axis, first, bands))
        first += bands

    def next_zone(value, along, steps):
        pairs = []
        zones = lax.axis_size("zone")
        for zone in range(zones - 1):
            for source, target in ring_pairs(along, steps, 0):
                pairs.append((zone * tile_count + source, (zone + 1) * tile_count + target))
        return lax.ppermute(value, ("zone", "tile"), pairs)

    near_list = passed_along(seam_list, "zone", 1)
    near_list_by = {axis: next_zone(seam_list, axis, 1) for axis in ("x", "z")}
    list_by = {axis: hop(seam_list, axis, 1) for axis in ("x", "z")}

    nears, beyonds, nears_beyond = [], [], []
    for part, (axis, first, bands) in enumerate(parts):
        nears.append(passed_along(pick(seam_list, tiles, first, bands), "zone", 1))
        beyonds.append(hop(tiles[:, first : first + bands], axis, 1))
        if part == 0:
            nears_beyond.append(hop(nears[0], axis, 1))
        else:
            nears_beyond.append(passed_along(pick(list_by[axis], beyonds[part], 0, bands), "zone", 1))

    def coordinates(device):
        return device // (2 * RING), (device // 2) % RING, device % 2

    order_ids = jnp.arange(per_owner, dtype=jnp.int32)
    owner_ids = jnp.arange(tile_count, dtype=jnp.int32)
    src_device = (source // local_count).reshape(tile_count, per_owner)
    earlier = order_ids[None, :] < order_ids[:, None]
    owners_ahead = owner_ids[None, :] < owner_ids[:, None]
    same = src_device[:, :, None] == src_device[:, None, :]
    rank = jnp.sum((same & earlier[None]).astype(jnp.int32), axis=2)
    block_ids = owner_ids[:, None] * per_owner + order_ids[None, :]
    my_x, my_z, my_core = coordinates(myself)
    src_x, src_z, src_core = coordinates(src_device)
    own_x, own_z, own_core = coordinates(owner_ids[:, None])
    own_src = lax.dynamic_index_in_dim(src_device, myself, 0, keepdims=False)
    own_rank = jnp.sum(((own_src[:, None] == own_src[None, :]) & earlier).astype(jnp.int32), axis=1)
    from_x, from_z, from_core = coordinates(own_src)

    def lists(my_p, my_q, src_p, src_q, own_p, own_q):
        behind = (my_p - src_p) & (RING - 1)
        ahead = (own_p - my_p) & (RING - 1)
        mine = (src_core == my_core) & (src_q == my_q)
        mine = mine & (((behind == 0) & ((ahead == 0) | (ahead == 3))) | ((behind == 1) & ((ahead == 0) | (ahead == 1))))
        lane = 2 * ((own_q - my_q) & (RING - 1)) + (own_core != my_core).astype(jnp.int32)
        slot = jnp.where(ahead == 0, 4 * lane + 2 * behind + rank, 2 * lane + rank)
        within = jnp.sum((mine[:, None, :] & earlier[None]).astype(jnp.int32), axis=2)
        each = jnp.sum(mine.astype(jnp.int32), axis=1)
        turn = within + jnp.sum(jnp.where(owners_ahead, each[None, :], 0), axis=1)[:, None]
        hit = mine[None] & (turn[None] == jnp.arange(slots, dtype=jnp.int32)[:, None, None])

        def listed(values):
            return jnp.sum(jnp.where(hit, values[None], 0), axis=(1, 2))

        return jnp.sum(each)[None], listed(block_ids), listed(64 * ahead + slot), listed(behind)

    def taken(my_p, my_q, src_p, src_q):
        lane = 2 * ((my_q - src_q) & (RING - 1)) + (from_core != my_core).astype(jnp.int32)
        return lane, 2 * ((my_p - src_p) & (RING - 1)) + own_rank

    by_axis = {
        "x": lists(my_x, my_z, src_x, src_z, own_x, own_z),
        "z": lists(my_z, my_x, src_z, src_x, own_z, own_x),
    }
    picks = taken(my_x, my_z, from_x, from_z) + taken(my_z, my_x, from_z, from_x)
    taps = jnp.concatenate([cubic_weight(step - fractions[:, axis]) for axis in range(2) for step in STEPS])
    flat_offsets = offsets.reshape(-1)
    zone_flag = zone_index[None].astype(jnp.int32)
    listed_by = {axis: jnp.concatenate([near_list, near_list_by[axis], zone_flag]) for axis in ("x", "z")}

    arrays = []
    for part, (axis, first, bands) in enumerate(parts):
        scalars = by_axis[axis] + (source, flat_offsets, taps, blend, listed_by[axis])
        stay, up, down = render(scalars, tiles, beyonds[part], nears[part], nears_beyond[part], first)
        came_up, came_down = hop(up, axis, 1), hop(down, axis, -1)
        packed = pack(stay, came_up, came_down)
        other = "z" if axis == "x" else "x"
        arrays += [packed[0]] + [hop(packed[lane], other, lane // 2, lane % 2) for lane in range(1, LANES)]
    shape = (per_owner, band_count, height // 2, width // 2)
    return place(tuple(parts), picks, arrays, shape)


def solution(mesh):
    in_specs = (
        P(("zone", "tile"), None, None, None),
        P(("zone", "tile")),
        P("zone"),
        P("zone", None),
        P("zone", None),
        P("zone"),
    )
    out_specs = P(("zone", "tile"), None, None, None)
    return jax.shard_map(local, mesh=mesh, in_specs=in_specs, out_specs=out_specs, check_vma=False)
```

```python
import functools

import jax
import jax.numpy as jnp
from jax import lax
from jax.experimental import pallas as pl
from jax.experimental.pallas import tpu as pltpu
from jax.sharding import PartitionSpec as P


EARLY = 3
CHUNKS = (("x", 5), ("z", 5))
RING = 4
LANES = 2 * RING
ABREAST = 4
STEPS = (-1, 0, 1, 2)


def passed_along(value, axis, steps):
    count = lax.axis_size(axis)
    initial, last = (max(0, -steps), min(count, count - steps))
    return lax.ppermute(value, axis, [(source, source + steps) for source in range(initial, last)])


def cubic_weight(dist):
    mag = jnp.abs(dist)
    near = (1.5 * mag - 2.5) * mag * mag + 1.0
    far = ((-0.5 * mag + 2.5) * mag - 4.0) * mag + 2.0
    return jnp.where(mag <= 1.0, near, jnp.where(mag < 2.0, far, jnp.zeros_like(mag)))


def ring_pairs(along, steps, cross):
    pairs = []
    for x in range(RING):
        for z in range(RING):
            for core in range(2):
                to_x, to_z = ((x + steps) % RING, z) if along == "x" else (x, (z + steps) % RING)
                pairs.append(((x * RING + z) * 2 + core, (to_x * RING + to_z) * 2 + (core ^ cross)))
    return pairs


def hop(value, along, steps, cross=0):
    return lax.ppermute(value, "tile", ring_pairs(along, steps, cross))


def pick_kernel(first, bands, listed_ref, tiles_ref, picked_ref, held, in_sem, out_sem):
    count = picked_ref.shape[0]
    for index in range(count):
        pltpu.make_async_copy(
            tiles_ref.at[listed_ref[index], pl.ds(first, bands)], held.at[index], in_sem.at[index]
        ).start()
    for index in range(count):
        pltpu.make_async_copy(
            tiles_ref.at[listed_ref[index], pl.ds(first, bands)], held.at[index], in_sem.at[index]
        ).wait()
        pltpu.make_async_copy(held.at[index], picked_ref.at[index], out_sem.at[index]).start()
    for index in range(count):
        pltpu.make_async_copy(held.at[index], picked_ref.at[index], out_sem.at[index]).wait()


def pick(listed, tiles, first, bands):
    shape = (listed.shape[0], bands) + tiles.shape[2:]
    return pl.pallas_call(
        functools.partial(pick_kernel, first, bands),
        out_shape=jax.ShapeDtypeStruct(shape, tiles.dtype),
        in_specs=[pl.BlockSpec(memory_space=pltpu.SMEM), pl.BlockSpec(memory_space=pl.ANY)],
        out_specs=pl.BlockSpec(memory_space=pl.ANY),
        scratch_shapes=[
            pltpu.VMEM(shape, tiles.dtype),
            pltpu.SemaphoreType.DMA((shape[0],)),
            pltpu.SemaphoreType.DMA((shape[0],)),
        ],
        name="pick",
    )(listed, tiles)


def render_early_kernel(
    local_count, first, bands, seams, range_ref, blocks_ref, slots_ref, source_ref, offsets_ref, taps_ref, blend_ref,
    listed_ref, tiles_ref, *refs,
):
    if seams:
        near_ref, _, out_ref, held, beside, row_lag, col_lag, done, in_sem, out_sem = refs
        load_near = pltpu.make_async_copy(near_ref, beside, in_sem.at[1])
        load_near.start()
        start, stop = range_ref[0], range_ref[1]
    else:
        out_ref, held, row_lag, col_lag, done, in_sem, out_sem = refs
        start, stop = 0, range_ref[0]
    load = pltpu.make_async_copy(tiles_ref.at[:, pl.ds(first, bands)], held, in_sem.at[0])
    load.start()
    height, width = held.shape[2], held.shape[3]
    row_lag[...] = lax.broadcasted_iota(jnp.int32, row_lag.shape, 1) - 2 * lax.broadcasted_iota(jnp.int32, row_lag.shape, 0)
    col_lag[...] = lax.broadcasted_iota(jnp.int32, col_lag.shape, 0) - 2 * lax.broadcasted_iota(jnp.int32, col_lag.shape, 1)
    load.wait()
    if seams:
        load_near.wait()

    def store(index):
        way = lax.rem(index - start, 2 * ABREAST)
        return pltpu.make_async_copy(done.at[way], out_ref.at[slots_ref[index]], out_sem.at[way])

    def kernel_matrix(lag_ref, block, axis):
        lag = lag_ref[...] - offsets_ref[2 * block + axis]
        kernel = jnp.zeros(lag.shape, jnp.float32)
        for place, step in enumerate(STEPS):
            kernel = jnp.where(lag == step, taps_ref[(len(STEPS) * axis + place) * source_ref.shape[0] + block], kernel)
        return kernel.astype(jnp.bfloat16)

    def render_one(index):
        block = blocks_ref[index]
        tile = lax.rem(source_ref[block], local_count)
        row_kernel = kernel_matrix(row_lag, block, 0)
        col_kernel = kernel_matrix(col_lag, block, 1)
        if seams:
            place = jnp.where(listed_ref[1] == tile, 1, 0)
            weight = blend_ref[block]
            mixed = (1.0 - weight) * held[tile].astype(jnp.float32) + weight * beside[place].astype(jnp.float32)
            mixed = mixed.astype(jnp.bfloat16)
        else:
            mixed = held[tile]
        mixed = mixed.reshape(bands * height, width)
        across = jnp.dot(mixed, col_kernel, preferred_element_type=jnp.float32).astype(jnp.bfloat16)
        beside_each = jnp.concatenate([across[b * height : (b + 1) * height] for b in range(bands)], axis=1)
        return jnp.dot(row_kernel, beside_each, preferred_element_type=jnp.float32).astype(jnp.bfloat16)

    def some(turn, carry):
        begin = start + turn * ABREAST
        for ahead in range(ABREAST):

            @pl.when(turn >= 2)
            def _():
                store(begin + ahead - 2 * ABREAST).wait()

        results = [render_one(jnp.minimum(begin + ahead, stop - 1)) for ahead in range(ABREAST)]
        for ahead in range(ABREAST):
            way = lax.rem(turn, 2) * ABREAST + ahead
            for b in range(bands):
                done[way, b] = results[ahead][:, b * (width // 2) : (b + 1) * (width // 2)]
        for ahead in range(ABREAST):

            @pl.when(begin + ahead < stop)
            def _():
                store(begin + ahead).start()

        return carry

    turns = lax.div(stop - start + ABREAST - 1, ABREAST)
    lax.fori_loop(0, turns, some, 0)

    def drain(index, carry):
        store(index).wait()
        return carry

    lax.fori_loop(start + jnp.maximum(turns - 2, 0) * ABREAST, stop, drain, 0)


def render_early(scalars, tiles, first, bands, slots, near=None, begun=None):
    local_count, _, height, width = tiles.shape
    block = (bands, height // 2, width // 2)
    seams = near is not None
    arrays = (tiles, near, begun) if seams else (tiles,)
    flops = 12 * bands * (2 * height * width * width // 2 + height * width * height // 2)
    return pl.pallas_call(
        functools.partial(render_early_kernel, local_count, first, bands, seams),
        out_shape=jax.ShapeDtypeStruct((slots,) + block, jnp.bfloat16),
        in_specs=[pl.BlockSpec(memory_space=pltpu.SMEM)] * len(scalars)
        + [pl.BlockSpec(memory_space=pl.ANY)] * len(arrays),
        out_specs=pl.BlockSpec(memory_space=pl.ANY),
        scratch_shapes=[pltpu.VMEM((local_count, bands, height, width), jnp.bfloat16)]
        + ([pltpu.VMEM(near.shape, jnp.bfloat16)] if seams else [])
        + [
            pltpu.VMEM((height // 2, height), jnp.int32),
            pltpu.VMEM((width, width // 2), jnp.int32),
            pltpu.VMEM((2 * ABREAST,) + block, jnp.bfloat16),
            pltpu.SemaphoreType.DMA((2,)),
            pltpu.SemaphoreType.DMA((2 * ABREAST,)),
        ],
        input_output_aliases={len(scalars) + 2: 0} if seams else {},
        cost_estimate=pl.CostEstimate(flops=8 * flops, bytes_accessed=12 * bands * height * width // 2, transcendentals=0),
        name="early_seams" if seams else "early",
    )(*scalars, *arrays)


def swap(outgoing, capacity):
    slots = outgoing.shape[0]
    pairs = outgoing.reshape((slots // capacity, capacity) + outgoing.shape[1:])
    return lax.all_to_all(pairs, "tile", split_axis=0, concat_axis=0, tiled=True).reshape(outgoing.shape)


def render_kernel(
    local_count, first, bands, seams, range_ref, blocks_ref, into_ref, side_ref, source_ref, offsets_ref, taps_ref,
    blend_ref, listed_ref, tiles_ref, beyond_ref, *refs,
):
    if seams:
        near_ref, near_beyond_ref, _, _, _, stay_ref, up_ref, down_ref, held, beside = refs[:10]
        start, stop = range_ref[0], range_ref[1]
    else:
        stay_ref, up_ref, down_ref, held = refs[:4]
        start, stop = 0, range_ref[0]
    row_lag, col_lag, done, in_sem, out_sem = refs[-5:]
    loads = [
        pltpu.make_async_copy(tiles_ref.at[:, pl.ds(first, bands)], held.at[pl.ds(0, local_count)], in_sem.at[0]),
        pltpu.make_async_copy(beyond_ref, held.at[pl.ds(local_count, local_count)], in_sem.at[1]),
    ]
    if seams:
        listed = near_ref.shape[0]
        loads += [
            pltpu.make_async_copy(near_ref, beside.at[pl.ds(0, listed)], in_sem.at[2]),
            pltpu.make_async_copy(near_beyond_ref, beside.at[pl.ds(listed, listed)], in_sem.at[3]),
        ]
    for load in loads:
        load.start()
    height, width = held.shape[2], held.shape[3]
    row_lag[...] = lax.broadcasted_iota(jnp.int32, row_lag.shape, 1) - 2 * lax.broadcasted_iota(jnp.int32, row_lag.shape, 0)
    col_lag[...] = lax.broadcasted_iota(jnp.int32, col_lag.shape, 0) - 2 * lax.broadcasted_iota(jnp.int32, col_lag.shape, 1)
    for load in loads:
        load.wait()

    def start_store(index, way):
        into = into_ref[index]
        slot = lax.rem(into, 64)
        for number, out_ref in ((0, stay_ref), (1, up_ref), (3, down_ref)):

            @pl.when(lax.div(into, 64) == number)
            def _():
                pltpu.make_async_copy(done.at[way], out_ref.at[slot], out_sem.at[way]).start()

    def wait_store(way):
        pltpu.make_async_copy(done.at[way], stay_ref.at[0], out_sem.at[way]).wait()

    def kernel_matrix(lag_ref, block, axis):
        lag = lag_ref[...] - offsets_ref[2 * block + axis]
        kernel = jnp.zeros(lag.shape, jnp.float32)
        for place, step in enumerate(STEPS):
            kernel = jnp.where(lag == step, taps_ref[(len(STEPS) * axis + place) * source_ref.shape[0] + block], kernel)
        return kernel.astype(jnp.bfloat16)

    def render_one(index):
        block = blocks_ref[index]
        side = side_ref[index]
        tile = lax.rem(source_ref[block], local_count)
        row_kernel = kernel_matrix(row_lag, block, 0)
        col_kernel = kernel_matrix(col_lag, block, 1)
        mixed = held[local_count * side + tile]
        if seams:
            place = listed * side + jnp.where(listed_ref[listed * side + 1] == tile, 1, 0)
            weight = blend_ref[block]
            mixed = (1.0 - weight) * mixed.astype(jnp.float32) + weight * beside[place].astype(jnp.float32)
        mixed = mixed.astype(jnp.bfloat16).reshape(bands * height, width)
        across = jnp.dot(mixed, col_kernel, preferred_element_type=jnp.float32).astype(jnp.bfloat16)
        beside_each = jnp.concatenate([across[b * height : (b + 1) * height] for b in range(bands)], axis=1)
        return jnp.dot(row_kernel, beside_each, preferred_element_type=jnp.float32).astype(jnp.bfloat16)

    def some(turn, carry):
        begin = start + turn * ABREAST
        half = lax.rem(turn, 2) * ABREAST
        for ahead in range(ABREAST):

            @pl.when(turn >= 2)
            def _():
                wait_store(half + ahead)

        results = [render_one(jnp.minimum(begin + ahead, stop - 1)) for ahead in range(ABREAST)]
        for ahead in range(ABREAST):
            for b in range(bands):
                done[half + ahead, b] = results[ahead][:, b * (width // 2) : (b + 1) * (width // 2)]
        for ahead in range(ABREAST):

            @pl.when(begin + ahead < stop)
            def _():
                start_store(begin + ahead, half + ahead)

        return carry

    turns = lax.div(stop - start + ABREAST - 1, ABREAST)
    lax.fori_loop(0, turns, some, 0)

    def drain(index, carry):
        wait_store(lax.rem(index, 2 * ABREAST))
        return carry

    lax.fori_loop(jnp.maximum(turns - 2, 0) * ABREAST, stop - start, drain, 0)


def render(scalars, tiles, beyond, first, near=None, near_beyond=None, begun=()):
    local_count, _, height, width = tiles.shape
    bands = beyond.shape[1]
    block = (bands, height // 2, width // 2)
    seams = near is not None
    arrays = (tiles, beyond) + ((near, near_beyond) if seams else ()) + tuple(begun)
    flops = 12 * bands * (2 * height * width * width // 2 + height * width * height // 2)
    return pl.pallas_call(
        functools.partial(render_kernel, local_count, first, bands, seams),
        out_shape=[jax.ShapeDtypeStruct((slots,) + block, jnp.bfloat16) for slots in (4 * LANES, 2 * LANES, 2 * LANES)],
        in_specs=[pl.BlockSpec(memory_space=pltpu.SMEM)] * len(scalars)
        + [pl.BlockSpec(memory_space=pl.ANY)] * len(arrays),
        out_specs=[pl.BlockSpec(memory_space=pl.ANY)] * 3,
        scratch_shapes=[pltpu.VMEM((2 * local_count, bands, height, width), jnp.bfloat16)]
        + ([pltpu.VMEM((2 * near.shape[0], bands, height, width), jnp.bfloat16)] if seams else [])
        + [
            pltpu.VMEM((height // 2, height), jnp.int32),
            pltpu.VMEM((width, width // 2), jnp.int32),
            pltpu.VMEM((2 * ABREAST,) + block, jnp.bfloat16),
            pltpu.SemaphoreType.DMA((4,)),
            pltpu.SemaphoreType.DMA((2 * ABREAST,)),
        ],
        input_output_aliases={len(scalars) + 4 + number: number for number in range(3)} if seams else {},
        cost_estimate=pl.CostEstimate(flops=8 * flops, bytes_accessed=12 * bands * height * width // 2, transcendentals=0),
        name="late_seams" if seams else "late",
    )(*scalars, *arrays)


def pack_kernel(stay_ref, up_ref, down_ref, *refs):
    outs, (held, in_sem, out_sem) = refs[:LANES], refs[LANES:]
    copies = []
    for lane in range(LANES):
        copies += [
            pltpu.make_async_copy(stay_ref.at[pl.ds(4 * lane, 4)], held.at[lane, pl.ds(0, 4)], in_sem.at[lane, 0]),
            pltpu.make_async_copy(up_ref.at[pl.ds(2 * lane, 2)], held.at[lane, pl.ds(4, 2)], in_sem.at[lane, 1]),
            pltpu.make_async_copy(down_ref.at[pl.ds(2 * lane, 2)], held.at[lane, pl.ds(6, 2)], in_sem.at[lane, 2]),
        ]
    for copy in copies:
        copy.start()
    puts = [pltpu.make_async_copy(held.at[lane], outs[lane], out_sem.at[lane]) for lane in range(LANES)]
    for lane in range(LANES):
        for copy in copies[3 * lane : 3 * lane + 3]:
            copy.wait()
        puts[lane].start()
    for put in puts:
        put.wait()


def pack(stay, up, down):
    shape = (8,) + stay.shape[1:]
    return pl.pallas_call(
        pack_kernel,
        out_shape=[jax.ShapeDtypeStruct(shape, stay.dtype)] * LANES,
        in_specs=[pl.BlockSpec(memory_space=pl.ANY)] * 3,
        out_specs=[pl.BlockSpec(memory_space=pl.ANY)] * LANES,
        scratch_shapes=[
            pltpu.VMEM((LANES,) + shape, stay.dtype),
            pltpu.SemaphoreType.DMA((LANES, 3)),
            pltpu.SemaphoreType.DMA((LANES,)),
        ],
        name="pack",
    )(stay, up, down)


def place_kernel(parts, taken_ref, early_ref, x_lane_ref, x_slot_ref, z_lane_ref, z_slot_ref, *refs):
    arrays, (out_ref, held, in_sem, out_sem) = refs[: LANES * len(parts)], refs[LANES * len(parts) :]
    early = early_ref.shape[1]
    count = out_ref.shape[0]

    def take_early(index):
        return pltpu.make_async_copy(
            early_ref.at[taken_ref[index]], held.at[index, pl.ds(0, early)], in_sem.at[len(parts), index]
        )

    def take(index, carry):
        take_early(index).start()
        for number, (axis, first, bands) in enumerate(parts):
            lane_ref, slot_ref = (x_lane_ref, x_slot_ref) if axis == "x" else (z_lane_ref, z_slot_ref)
            for lane in range(LANES):

                @pl.when(lane_ref[index] == lane)
                def _():
                    pltpu.make_async_copy(
                        arrays[LANES * number + lane].at[slot_ref[index]],
                        held.at[index, pl.ds(first, bands)],
                        in_sem.at[number, index],
                    ).start()

        return carry

    lax.fori_loop(0, count, take, 0)

    def put(index, carry):
        take_early(index).wait()
        for number, (axis, first, bands) in enumerate(parts):
            pltpu.make_async_copy(
                arrays[LANES * number].at[0], held.at[index, pl.ds(first, bands)], in_sem.at[number, index]
            ).wait()
        pltpu.make_async_copy(held.at[index], out_ref.at[index], out_sem.at[index]).start()
        return carry

    lax.fori_loop(0, count, put, 0)

    def finish(index, carry):
        pltpu.make_async_copy(held.at[index], out_ref.at[index], out_sem.at[index]).wait()
        return carry

    lax.fori_loop(0, count, finish, 0)


def place(parts, taken, early, picks, arrays, shape):
    return pl.pallas_call(
        functools.partial(place_kernel, parts),
        out_shape=jax.ShapeDtypeStruct(shape, jnp.bfloat16),
        in_specs=[pl.BlockSpec(memory_space=pltpu.SMEM), pl.BlockSpec(memory_space=pl.ANY)]
        + [pl.BlockSpec(memory_space=pltpu.SMEM)] * 4
        + [pl.BlockSpec(memory_space=pl.ANY)] * len(arrays),
        out_specs=pl.BlockSpec(memory_space=pl.ANY),
        scratch_shapes=[
            pltpu.VMEM(shape, jnp.bfloat16),
            pltpu.SemaphoreType.DMA((len(parts) + 1, shape[0])),
            pltpu.SemaphoreType.DMA((shape[0],)),
        ],
        name="place",
    )(taken, early, *picks, *arrays)


def local(tiles, seam_list, source, offsets, fractions, blend):
    tile_count = lax.axis_size("tile")
    myself = lax.axis_index("tile")
    zone_index = lax.axis_index("zone")
    local_count, band_count, height, width = tiles.shape
    per_owner = source.shape[0] // tile_count
    slots = 8 * LANES

    parts, first = [], EARLY
    for axis, bands in CHUNKS:
        parts.append((axis, first, bands))
        first += bands

    def next_zone(value, along, steps):
        pairs = []
        zones = lax.axis_size("zone")
        for zone in range(zones - 1):
            for source, target in ring_pairs(along, steps, 0):
                pairs.append((zone * tile_count + source, (zone + 1) * tile_count + target))
        return lax.ppermute(value, ("zone", "tile"), pairs)

    near_list = passed_along(seam_list, "zone", 1)
    near_list_by = {axis: next_zone(seam_list, axis, 1) for axis in ("x", "z")}
    list_by = {axis: hop(seam_list, axis, 1) for axis in ("x", "z")}

    near_early = passed_along(pick(seam_list, tiles, 0, EARLY), "zone", 1)
    nears, beyonds, nears_beyond = [], [], []
    for part, (axis, first, bands) in enumerate(parts):
        nears.append(passed_along(pick(seam_list, tiles, first, bands), "zone", 1))
        beyonds.append(hop(tiles[:, first : first + bands], axis, 1))
        nears_beyond.append(passed_along(pick(list_by[axis], beyonds[part], 0, bands), "zone", 1))

    def coordinates(device):
        return device // (2 * RING), (device // 2) % RING, device % 2

    order_ids = jnp.arange(per_owner, dtype=jnp.int32)
    owner_ids = jnp.arange(tile_count, dtype=jnp.int32)
    src_device = (source // local_count).reshape(tile_count, per_owner)
    earlier = order_ids[None, :] < order_ids[:, None]
    owners_ahead = owner_ids[None, :] < owner_ids[:, None]
    same = src_device[:, :, None] == src_device[:, None, :]
    rank = jnp.sum((same & earlier[None]).astype(jnp.int32), axis=2)
    block_ids = owner_ids[:, None] * per_owner + order_ids[None, :]
    my_x, my_z, my_core = coordinates(myself)
    src_x, src_z, src_core = coordinates(src_device)
    own_x, own_z, own_core = coordinates(owner_ids[:, None])
    own_src = lax.dynamic_index_in_dim(src_device, myself, 0, keepdims=False)
    own_rank = jnp.sum(((own_src[:, None] == own_src[None, :]) & earlier).astype(jnp.int32), axis=1)
    from_x, from_z, from_core = coordinates(own_src)

    tile_of = (source % local_count).reshape(tile_count, per_owner)
    in_next = zone_index > 0

    def in_list(device_list):
        return jnp.any(tile_of[:, :, None] == device_list[None, None, :], axis=2) & in_next

    def line(plain, flagged, values):
        def place_in_line(members):
            within = jnp.sum((members[:, None, :] & earlier[None]).astype(jnp.int32), axis=2)
            each = jnp.sum(members.astype(jnp.int32), axis=1)
            return within + jnp.sum(jnp.where(owners_ahead, each[None, :], 0), axis=1)[:, None], jnp.sum(each)

        plain_turn, plain_count = place_in_line(plain)
        seam_turn, seam_count = place_in_line(flagged)
        turn = jnp.where(plain, plain_turn, jnp.where(flagged, plain_count + seam_turn, -1))
        hit = turn[None] == jnp.arange(slots, dtype=jnp.int32)[:, None, None]
        listed = tuple(jnp.sum(jnp.where(hit, value[None], 0), axis=(1, 2)) for value in values)
        return (jnp.stack([plain_count, plain_count + seam_count]),) + listed

    taps = jnp.concatenate([cubic_weight(step - fractions[:, axis]) for axis in range(2) for step in STEPS])
    flat_offsets = offsets.reshape(-1)
    mine = src_device == myself
    flags = in_list(near_list)
    early_list = line(mine & ~flags, mine & flags, (block_ids, 2 * owner_ids[:, None] + rank))
    scalars = early_list + (source, flat_offsets, taps, blend, near_list)
    outgoing = render_early(scalars, tiles, 0, EARLY, slots)
    outgoing = render_early(scalars, tiles, 0, EARLY, slots, near_early, outgoing)
    early = swap(outgoing, 2)
    outgoing, src_device, rank, block_ids, own_src = lax.optimization_barrier(
        (outgoing, src_device, rank, block_ids, own_src)
    )
    src_x, src_z, src_core = coordinates(src_device)
    from_x, from_z, from_core = coordinates(own_src)

    def lists(my_p, my_q, src_p, src_q, own_p, own_q, lists_by_side):
        behind = (my_p - src_p) & (RING - 1)
        ahead = (own_p - my_p) & (RING - 1)
        mine = (src_core == my_core) & (src_q == my_q)
        mine = mine & (((behind == 0) & ((ahead == 0) | (ahead == 3))) | ((behind == 1) & ((ahead == 0) | (ahead == 1))))
        lane = 2 * ((own_q - my_q) & (RING - 1)) + (own_core != my_core).astype(jnp.int32)
        slot = jnp.where(ahead == 0, 4 * lane + 2 * behind + rank, 2 * lane + rank)
        flags = jnp.where(behind == 0, in_list(lists_by_side[0]), in_list(lists_by_side[1]))
        return line(mine & ~flags, mine & flags, (block_ids, 64 * ahead + slot, behind))

    def taken(my_p, my_q, src_p, src_q):
        lane = 2 * ((my_q - src_q) & (RING - 1)) + (from_core != my_core).astype(jnp.int32)
        return lane, 2 * ((my_p - src_p) & (RING - 1)) + own_rank

    by_axis = {
        "x": lists(my_x, my_z, src_x, src_z, own_x, own_z, (near_list, near_list_by["x"])),
        "z": lists(my_z, my_x, src_z, src_x, own_z, own_x, (near_list, near_list_by["z"])),
    }
    picks = taken(my_x, my_z, from_x, from_z) + taken(my_z, my_x, from_z, from_x)
    listed_by = {axis: jnp.concatenate([near_list, near_list_by[axis]]) for axis in ("x", "z")}

    begun = []
    for part, (axis, first, bands) in enumerate(parts):
        scalars = by_axis[axis] + (source, flat_offsets, taps, blend, listed_by[axis])
        begun.append(render(scalars, tiles, beyonds[part], first))
    arrays = []
    for part, (axis, first, bands) in enumerate(parts):
        scalars = by_axis[axis] + (source, flat_offsets, taps, blend, listed_by[axis])
        stay, up, down = render(scalars, tiles, beyonds[part], first, nears[part], nears_beyond[part], begun[part])
        came_up, came_down = hop(up, axis, 1), hop(down, axis, -1)
        packed = pack(stay, came_up, came_down)
        other = "z" if axis == "x" else "x"
        arrays += [packed[0]] + [hop(packed[lane], other, lane // 2, lane % 2) for lane in range(1, LANES)]
    shape = (per_owner, band_count, height // 2, width // 2)
    own_taken = 2 * own_src + own_rank
    return place(tuple(parts), own_taken, early, picks, arrays, shape)


def solution(mesh):
    in_specs = (
        P(("zone", "tile"), None, None, None),
        P(("zone", "tile")),
        P("zone"),
        P("zone", None),
        P("zone", None),
        P("zone"),
    )
    out_specs = P(("zone", "tile"), None, None, None)
    return jax.shard_map(local, mesh=mesh, in_specs=in_specs, out_specs=out_specs, check_vma=False)
```

```python
import functools

import jax
import jax.numpy as jnp
from jax import lax
from jax.experimental import pallas as pl
from jax.experimental.pallas import tpu as pltpu
from jax.sharding import PartitionSpec as P


EARLY = 3
CHUNKS = (("x", 6), ("z", 4))
RING = 4
LANES = 2 * RING
ABREAST = 4
STEPS = (-1, 0, 1, 2)


def passed_along(value, axis, steps):
    count = lax.axis_size(axis)
    initial, last = (max(0, -steps), min(count, count - steps))
    return lax.ppermute(value, axis, [(source, source + steps) for source in range(initial, last)])


def cubic_weight(dist):
    mag = jnp.abs(dist)
    near = (1.5 * mag - 2.5) * mag * mag + 1.0
    far = ((-0.5 * mag + 2.5) * mag - 4.0) * mag + 2.0
    return jnp.where(mag <= 1.0, near, jnp.where(mag < 2.0, far, jnp.zeros_like(mag)))


def ring_pairs(along, steps, cross):
    pairs = []
    for x in range(RING):
        for z in range(RING):
            for core in range(2):
                to_x, to_z = ((x + steps) % RING, z) if along == "x" else (x, (z + steps) % RING)
                pairs.append(((x * RING + z) * 2 + core, (to_x * RING + to_z) * 2 + (core ^ cross)))
    return pairs


def hop(value, along, steps, cross=0):
    return lax.ppermute(value, "tile", ring_pairs(along, steps, cross))


def pick_kernel(first, bands, listed_ref, tiles_ref, picked_ref, held, in_sem, out_sem):
    count = picked_ref.shape[0]
    for index in range(count):
        pltpu.make_async_copy(
            tiles_ref.at[listed_ref[index], pl.ds(first, bands)], held.at[index], in_sem.at[index]
        ).start()
    for index in range(count):
        pltpu.make_async_copy(
            tiles_ref.at[listed_ref[index], pl.ds(first, bands)], held.at[index], in_sem.at[index]
        ).wait()
        pltpu.make_async_copy(held.at[index], picked_ref.at[index], out_sem.at[index]).start()
    for index in range(count):
        pltpu.make_async_copy(held.at[index], picked_ref.at[index], out_sem.at[index]).wait()


def pick(listed, tiles, first, bands):
    shape = (listed.shape[0], bands) + tiles.shape[2:]
    return pl.pallas_call(
        functools.partial(pick_kernel, first, bands),
        out_shape=jax.ShapeDtypeStruct(shape, tiles.dtype),
        in_specs=[pl.BlockSpec(memory_space=pltpu.SMEM), pl.BlockSpec(memory_space=pl.ANY)],
        out_specs=pl.BlockSpec(memory_space=pl.ANY),
        scratch_shapes=[
            pltpu.VMEM(shape, tiles.dtype),
            pltpu.SemaphoreType.DMA((shape[0],)),
            pltpu.SemaphoreType.DMA((shape[0],)),
        ],
        name="pick",
    )(listed, tiles)


def render_early_kernel(
    local_count, first, bands, seams, range_ref, blocks_ref, slots_ref, source_ref, offsets_ref, taps_ref, blend_ref,
    listed_ref, tiles_ref, *refs,
):
    if seams:
        near_ref, _, out_ref, held, beside, row_lag, col_lag, done, in_sem, out_sem = refs
        load_near = pltpu.make_async_copy(near_ref, beside, in_sem.at[1])
        load_near.start()
        start, stop = range_ref[0], range_ref[1]
    else:
        out_ref, held, row_lag, col_lag, done, in_sem, out_sem = refs
        start, stop = 0, range_ref[0]
    load = pltpu.make_async_copy(tiles_ref.at[:, pl.ds(first, bands)], held, in_sem.at[0])
    load.start()
    height, width = held.shape[2], held.shape[3]
    row_lag[...] = lax.broadcasted_iota(jnp.int32, row_lag.shape, 1) - 2 * lax.broadcasted_iota(jnp.int32, row_lag.shape, 0)
    col_lag[...] = lax.broadcasted_iota(jnp.int32, col_lag.shape, 0) - 2 * lax.broadcasted_iota(jnp.int32, col_lag.shape, 1)
    load.wait()
    if seams:
        load_near.wait()

    def store(index):
        way = lax.rem(index - start, 2 * ABREAST)
        return pltpu.make_async_copy(done.at[way], out_ref.at[slots_ref[index]], out_sem.at[way])

    def kernel_matrix(lag_ref, block, axis):
        lag = lag_ref[...] - offsets_ref[2 * block + axis]
        kernel = jnp.zeros(lag.shape, jnp.float32)
        for place, step in enumerate(STEPS):
            kernel = jnp.where(lag == step, taps_ref[(len(STEPS) * axis + place) * source_ref.shape[0] + block], kernel)
        return kernel.astype(jnp.bfloat16)

    def render_one(index):
        block = blocks_ref[index]
        tile = lax.rem(source_ref[block], local_count)
        row_kernel = kernel_matrix(row_lag, block, 0)
        col_kernel = kernel_matrix(col_lag, block, 1)
        if seams:
            place = jnp.where(listed_ref[1] == tile, 1, 0)
            weight = blend_ref[block]
            mixed = (1.0 - weight) * held[tile].astype(jnp.float32) + weight * beside[place].astype(jnp.float32)
            mixed = mixed.astype(jnp.bfloat16)
        else:
            mixed = held[tile]
        mixed = mixed.reshape(bands * height, width)
        across = jnp.dot(mixed, col_kernel, preferred_element_type=jnp.float32).astype(jnp.bfloat16)
        beside_each = jnp.concatenate([across[b * height : (b + 1) * height] for b in range(bands)], axis=1)
        return jnp.dot(row_kernel, beside_each, preferred_element_type=jnp.float32).astype(jnp.bfloat16)

    def some(turn, carry):
        begin = start + turn * ABREAST
        for ahead in range(ABREAST):

            @pl.when(turn >= 2)
            def _():
                store(begin + ahead - 2 * ABREAST).wait()

        results = [render_one(jnp.minimum(begin + ahead, stop - 1)) for ahead in range(ABREAST)]
        for ahead in range(ABREAST):
            way = lax.rem(turn, 2) * ABREAST + ahead
            for b in range(bands):
                done[way, b] = results[ahead][:, b * (width // 2) : (b + 1) * (width // 2)]
        for ahead in range(ABREAST):

            @pl.when(begin + ahead < stop)
            def _():
                store(begin + ahead).start()

        return carry

    turns = lax.div(stop - start + ABREAST - 1, ABREAST)
    lax.fori_loop(0, turns, some, 0)

    def drain(index, carry):
        store(index).wait()
        return carry

    lax.fori_loop(start + jnp.maximum(turns - 2, 0) * ABREAST, stop, drain, 0)


def render_early(scalars, tiles, first, bands, slots, near=None, begun=None):
    local_count, _, height, width = tiles.shape
    block = (bands, height // 2, width // 2)
    seams = near is not None
    arrays = (tiles, near, begun) if seams else (tiles,)
    flops = 12 * bands * (2 * height * width * width // 2 + height * width * height // 2)
    return pl.pallas_call(
        functools.partial(render_early_kernel, local_count, first, bands, seams),
        out_shape=jax.ShapeDtypeStruct((slots,) + block, jnp.bfloat16),
        in_specs=[pl.BlockSpec(memory_space=pltpu.SMEM)] * len(scalars)
        + [pl.BlockSpec(memory_space=pl.ANY)] * len(arrays),
        out_specs=pl.BlockSpec(memory_space=pl.ANY),
        scratch_shapes=[pltpu.VMEM((local_count, bands, height, width), jnp.bfloat16)]
        + ([pltpu.VMEM(near.shape, jnp.bfloat16)] if seams else [])
        + [
            pltpu.VMEM((height // 2, height), jnp.int32),
            pltpu.VMEM((width, width // 2), jnp.int32),
            pltpu.VMEM((2 * ABREAST,) + block, jnp.bfloat16),
            pltpu.SemaphoreType.DMA((2,)),
            pltpu.SemaphoreType.DMA((2 * ABREAST,)),
        ],
        input_output_aliases={len(scalars) + 2: 0} if seams else {},
        cost_estimate=pl.CostEstimate(flops=8 * flops, bytes_accessed=12 * bands * height * width // 2, transcendentals=0),
        name="early_seams" if seams else "early",
    )(*scalars, *arrays)


def swap(outgoing, capacity):
    slots = outgoing.shape[0]
    pairs = outgoing.reshape((slots // capacity, capacity) + outgoing.shape[1:])
    return lax.all_to_all(pairs, "tile", split_axis=0, concat_axis=0, tiled=True).reshape(outgoing.shape)


def render_kernel(
    local_count, first, bands, seams, range_ref, blocks_ref, into_ref, side_ref, source_ref, offsets_ref, taps_ref,
    blend_ref, listed_ref, tiles_ref, beyond_ref, *refs,
):
    if seams:
        near_ref, near_beyond_ref, _, _, _, stay_ref, up_ref, down_ref, held, beside = refs[:10]
        start, stop = range_ref[0], range_ref[1]
    else:
        stay_ref, up_ref, down_ref, held = refs[:4]
        start, stop = 0, range_ref[0]
    row_lag, col_lag, done, in_sem, out_sem = refs[-5:]
    loads = [
        pltpu.make_async_copy(tiles_ref.at[:, pl.ds(first, bands)], held.at[pl.ds(0, local_count)], in_sem.at[0]),
        pltpu.make_async_copy(beyond_ref, held.at[pl.ds(local_count, local_count)], in_sem.at[1]),
    ]
    if seams:
        listed = near_ref.shape[0]
        loads += [
            pltpu.make_async_copy(near_ref, beside.at[pl.ds(0, listed)], in_sem.at[2]),
            pltpu.make_async_copy(near_beyond_ref, beside.at[pl.ds(listed, listed)], in_sem.at[3]),
        ]
    for load in loads:
        load.start()
    height, width = held.shape[2], held.shape[3]
    row_lag[...] = lax.broadcasted_iota(jnp.int32, row_lag.shape, 1) - 2 * lax.broadcasted_iota(jnp.int32, row_lag.shape, 0)
    col_lag[...] = lax.broadcasted_iota(jnp.int32, col_lag.shape, 0) - 2 * lax.broadcasted_iota(jnp.int32, col_lag.shape, 1)
    for load in loads:
        load.wait()

    def start_store(index, way):
        into = into_ref[index]
        slot = lax.rem(into, 64)
        for number, out_ref in ((0, stay_ref), (1, up_ref), (3, down_ref)):

            @pl.when(lax.div(into, 64) == number)
            def _():
                pltpu.make_async_copy(done.at[way], out_ref.at[slot], out_sem.at[way]).start()

    def wait_store(way):
        pltpu.make_async_copy(done.at[way], stay_ref.at[0], out_sem.at[way]).wait()

    def kernel_matrix(lag_ref, block, axis):
        lag = lag_ref[...] - offsets_ref[2 * block + axis]
        kernel = jnp.zeros(lag.shape, jnp.float32)
        for place, step in enumerate(STEPS):
            kernel = jnp.where(lag == step, taps_ref[(len(STEPS) * axis + place) * source_ref.shape[0] + block], kernel)
        return kernel.astype(jnp.bfloat16)

    def render_one(index):
        block = blocks_ref[index]
        side = side_ref[index]
        tile = lax.rem(source_ref[block], local_count)
        row_kernel = kernel_matrix(row_lag, block, 0)
        col_kernel = kernel_matrix(col_lag, block, 1)
        mixed = held[local_count * side + tile]
        if seams:
            place = listed * side + jnp.where(listed_ref[listed * side + 1] == tile, 1, 0)
            weight = blend_ref[block]
            mixed = (1.0 - weight) * mixed.astype(jnp.float32) + weight * beside[place].astype(jnp.float32)
        mixed = mixed.astype(jnp.bfloat16).reshape(bands * height, width)
        across = jnp.dot(mixed, col_kernel, preferred_element_type=jnp.float32).astype(jnp.bfloat16)
        beside_each = jnp.concatenate([across[b * height : (b + 1) * height] for b in range(bands)], axis=1)
        return jnp.dot(row_kernel, beside_each, preferred_element_type=jnp.float32).astype(jnp.bfloat16)

    def some(turn, carry):
        begin = start + turn * ABREAST
        half = lax.rem(turn, 2) * ABREAST
        for ahead in range(ABREAST):

            @pl.when(turn >= 2)
            def _():
                wait_store(half + ahead)

        results = [render_one(jnp.minimum(begin + ahead, stop - 1)) for ahead in range(ABREAST)]
        for ahead in range(ABREAST):
            for b in range(bands):
                done[half + ahead, b] = results[ahead][:, b * (width // 2) : (b + 1) * (width // 2)]
        for ahead in range(ABREAST):

            @pl.when(begin + ahead < stop)
            def _():
                start_store(begin + ahead, half + ahead)

        return carry

    turns = lax.div(stop - start + ABREAST - 1, ABREAST)
    lax.fori_loop(0, turns, some, 0)

    def drain(index, carry):
        wait_store(lax.rem(index, 2 * ABREAST))
        return carry

    lax.fori_loop(jnp.maximum(turns - 2, 0) * ABREAST, stop - start, drain, 0)


def render(scalars, tiles, beyond, first, near=None, near_beyond=None, begun=()):
    local_count, _, height, width = tiles.shape
    bands = beyond.shape[1]
    block = (bands, height // 2, width // 2)
    seams = near is not None
    arrays = (tiles, beyond) + ((near, near_beyond) if seams else ()) + tuple(begun)
    flops = 12 * bands * (2 * height * width * width // 2 + height * width * height // 2)
    return pl.pallas_call(
        functools.partial(render_kernel, local_count, first, bands, seams),
        out_shape=[jax.ShapeDtypeStruct((slots,) + block, jnp.bfloat16) for slots in (4 * LANES, 2 * LANES, 2 * LANES)],
        in_specs=[pl.BlockSpec(memory_space=pltpu.SMEM)] * len(scalars)
        + [pl.BlockSpec(memory_space=pl.ANY)] * len(arrays),
        out_specs=[pl.BlockSpec(memory_space=pl.ANY)] * 3,
        scratch_shapes=[pltpu.VMEM((2 * local_count, bands, height, width), jnp.bfloat16)]
        + ([pltpu.VMEM((2 * near.shape[0], bands, height, width), jnp.bfloat16)] if seams else [])
        + [
            pltpu.VMEM((height // 2, height), jnp.int32),
            pltpu.VMEM((width, width // 2), jnp.int32),
            pltpu.VMEM((2 * ABREAST,) + block, jnp.bfloat16),
            pltpu.SemaphoreType.DMA((4,)),
            pltpu.SemaphoreType.DMA((2 * ABREAST,)),
        ],
        input_output_aliases={len(scalars) + 4 + number: number for number in range(3)} if seams else {},
        cost_estimate=pl.CostEstimate(flops=8 * flops, bytes_accessed=12 * bands * height * width // 2, transcendentals=0),
        name="late_seams" if seams else "late",
    )(*scalars, *arrays)


def pack_kernel(stay_ref, up_ref, down_ref, *refs):
    outs, (held, in_sem, out_sem) = refs[:LANES], refs[LANES:]
    copies = []
    for lane in range(LANES):
        copies += [
            pltpu.make_async_copy(stay_ref.at[pl.ds(4 * lane, 4)], held.at[lane, pl.ds(0, 4)], in_sem.at[lane, 0]),
            pltpu.make_async_copy(up_ref.at[pl.ds(2 * lane, 2)], held.at[lane, pl.ds(4, 2)], in_sem.at[lane, 1]),
            pltpu.make_async_copy(down_ref.at[pl.ds(2 * lane, 2)], held.at[lane, pl.ds(6, 2)], in_sem.at[lane, 2]),
        ]
    for copy in copies:
        copy.start()
    puts = [pltpu.make_async_copy(held.at[lane], outs[lane], out_sem.at[lane]) for lane in range(LANES)]
    for lane in range(LANES):
        for copy in copies[3 * lane : 3 * lane + 3]:
            copy.wait()
        puts[lane].start()
    for put in puts:
        put.wait()


def pack(stay, up, down):
    shape = (8,) + stay.shape[1:]
    return pl.pallas_call(
        pack_kernel,
        out_shape=[jax.ShapeDtypeStruct(shape, stay.dtype)] * LANES,
        in_specs=[pl.BlockSpec(memory_space=pl.ANY)] * 3,
        out_specs=[pl.BlockSpec(memory_space=pl.ANY)] * LANES,
        scratch_shapes=[
            pltpu.VMEM((LANES,) + shape, stay.dtype),
            pltpu.SemaphoreType.DMA((LANES, 3)),
            pltpu.SemaphoreType.DMA((LANES,)),
        ],
        name="pack",
    )(stay, up, down)


def place_kernel(parts, taken_ref, early_ref, x_lane_ref, x_slot_ref, z_lane_ref, z_slot_ref, *refs):
    arrays, (out_ref, held, in_sem, out_sem) = refs[: LANES * len(parts)], refs[LANES * len(parts) :]
    early = early_ref.shape[1]
    count = out_ref.shape[0]

    def take_early(index):
        return pltpu.make_async_copy(
            early_ref.at[taken_ref[index]], held.at[index, pl.ds(0, early)], in_sem.at[len(parts), index]
        )

    def take(index, carry):
        take_early(index).start()
        for number, (axis, first, bands) in enumerate(parts):
            lane_ref, slot_ref = (x_lane_ref, x_slot_ref) if axis == "x" else (z_lane_ref, z_slot_ref)
            for lane in range(LANES):

                @pl.when(lane_ref[index] == lane)
                def _():
                    pltpu.make_async_copy(
                        arrays[LANES * number + lane].at[slot_ref[index]],
                        held.at[index, pl.ds(first, bands)],
                        in_sem.at[number, index],
                    ).start()

        return carry

    lax.fori_loop(0, count, take, 0)

    def put(index, carry):
        take_early(index).wait()
        for number, (axis, first, bands) in enumerate(parts):
            pltpu.make_async_copy(
                arrays[LANES * number].at[0], held.at[index, pl.ds(first, bands)], in_sem.at[number, index]
            ).wait()
        pltpu.make_async_copy(held.at[index], out_ref.at[index], out_sem.at[index]).start()
        return carry

    lax.fori_loop(0, count, put, 0)

    def finish(index, carry):
        pltpu.make_async_copy(held.at[index], out_ref.at[index], out_sem.at[index]).wait()
        return carry

    lax.fori_loop(0, count, finish, 0)


def place(parts, taken, early, picks, arrays, shape):
    return pl.pallas_call(
        functools.partial(place_kernel, parts),
        out_shape=jax.ShapeDtypeStruct(shape, jnp.bfloat16),
        in_specs=[pl.BlockSpec(memory_space=pltpu.SMEM), pl.BlockSpec(memory_space=pl.ANY)]
        + [pl.BlockSpec(memory_space=pltpu.SMEM)] * 4
        + [pl.BlockSpec(memory_space=pl.ANY)] * len(arrays),
        out_specs=pl.BlockSpec(memory_space=pl.ANY),
        scratch_shapes=[
            pltpu.VMEM(shape, jnp.bfloat16),
            pltpu.SemaphoreType.DMA((len(parts) + 1, shape[0])),
            pltpu.SemaphoreType.DMA((shape[0],)),
        ],
        name="place",
    )(taken, early, *picks, *arrays)


def local(tiles, seam_list, source, offsets, fractions, blend):
    tile_count = lax.axis_size("tile")
    myself = lax.axis_index("tile")
    zone_index = lax.axis_index("zone")
    local_count, band_count, height, width = tiles.shape
    per_owner = source.shape[0] // tile_count
    slots = 8 * LANES

    parts, first = [], EARLY
    for axis, bands in CHUNKS:
        parts.append((axis, first, bands))
        first += bands

    near_list = passed_along(seam_list, "zone", 1)
    near_early = passed_along(pick(seam_list, tiles, 0, EARLY), "zone", 1)
    both = {axis: hop(jnp.concatenate([seam_list, near_list]), axis, 1) for axis in ("x", "z")}
    list_by = {axis: lists[: seam_list.shape[0]] for axis, lists in both.items()}
    near_list_by = {axis: lists[seam_list.shape[0] :] for axis, lists in both.items()}
    nears, beyonds, nears_beyond = [], [], []
    for part, (axis, first, bands) in enumerate(parts):
        nears.append(passed_along(pick(seam_list, tiles, first, bands), "zone", 1))
        beyonds.append(hop(tiles[:, first : first + bands], axis, 1))
        nears_beyond.append(passed_along(pick(list_by[axis], beyonds[part], 0, bands), "zone", 1))

    def coordinates(device):
        return device // (2 * RING), (device // 2) % RING, device % 2

    order_ids = jnp.arange(per_owner, dtype=jnp.int32)
    owner_ids = jnp.arange(tile_count, dtype=jnp.int32)
    src_device = (source // local_count).reshape(tile_count, per_owner)
    earlier = order_ids[None, :] < order_ids[:, None]
    owners_ahead = owner_ids[None, :] < owner_ids[:, None]
    same = src_device[:, :, None] == src_device[:, None, :]
    rank = jnp.sum((same & earlier[None]).astype(jnp.int32), axis=2)
    block_ids = owner_ids[:, None] * per_owner + order_ids[None, :]
    my_x, my_z, my_core = coordinates(myself)
    src_x, src_z, src_core = coordinates(src_device)
    own_x, own_z, own_core = coordinates(owner_ids[:, None])
    own_src = lax.dynamic_index_in_dim(src_device, myself, 0, keepdims=False)
    own_rank = jnp.sum(((own_src[:, None] == own_src[None, :]) & earlier).astype(jnp.int32), axis=1)
    from_x, from_z, from_core = coordinates(own_src)

    tile_of = (source % local_count).reshape(tile_count, per_owner)
    in_next = zone_index > 0

    def in_list(device_list):
        return jnp.any(tile_of[:, :, None] == device_list[None, None, :], axis=2) & in_next

    def line(plain, flagged, values):
        def place_in_line(members):
            within = jnp.sum((members[:, None, :] & earlier[None]).astype(jnp.int32), axis=2)
            each = jnp.sum(members.astype(jnp.int32), axis=1)
            return within + jnp.sum(jnp.where(owners_ahead, each[None, :], 0), axis=1)[:, None], jnp.sum(each)

        plain_turn, plain_count = place_in_line(plain)
        seam_turn, seam_count = place_in_line(flagged)
        turn = jnp.where(plain, plain_turn, jnp.where(flagged, plain_count + seam_turn, -1))
        hit = turn[None] == jnp.arange(slots, dtype=jnp.int32)[:, None, None]
        listed = tuple(jnp.sum(jnp.where(hit, value[None], 0), axis=(1, 2)) for value in values)
        return (jnp.stack([plain_count, plain_count + seam_count]),) + listed

    taps = jnp.concatenate([cubic_weight(step - fractions[:, axis]) for axis in range(2) for step in STEPS])
    flat_offsets = offsets.reshape(-1)
    mine = src_device == myself
    flags = in_list(near_list)
    early_list = line(mine & ~flags, mine & flags, (block_ids, 2 * owner_ids[:, None] + rank))
    scalars = early_list + (source, flat_offsets, taps, blend, near_list)
    outgoing = render_early(scalars, tiles, 0, EARLY, slots)
    outgoing = render_early(scalars, tiles, 0, EARLY, slots, near_early, outgoing)
    early = swap(outgoing, 2)
    outgoing, src_device, rank, block_ids, own_src = lax.optimization_barrier(
        (outgoing, src_device, rank, block_ids, own_src)
    )
    src_x, src_z, src_core = coordinates(src_device)
    from_x, from_z, from_core = coordinates(own_src)

    def lists(my_p, my_q, src_p, src_q, own_p, own_q, lists_by_side):
        behind = (my_p - src_p) & (RING - 1)
        ahead = (own_p - my_p) & (RING - 1)
        mine = (src_core == my_core) & (src_q == my_q)
        mine = mine & (((behind == 0) & ((ahead == 0) | (ahead == 3))) | ((behind == 1) & ((ahead == 0) | (ahead == 1))))
        lane = 2 * ((own_q - my_q) & (RING - 1)) + (own_core != my_core).astype(jnp.int32)
        slot = jnp.where(ahead == 0, 4 * lane + 2 * behind + rank, 2 * lane + rank)
        flags = jnp.where(behind == 0, in_list(lists_by_side[0]), in_list(lists_by_side[1]))
        return line(mine & ~flags, mine & flags, (block_ids, 64 * ahead + slot, behind))

    def taken(my_p, my_q, src_p, src_q):
        lane = 2 * ((my_q - src_q) & (RING - 1)) + (from_core != my_core).astype(jnp.int32)
        return lane, 2 * ((my_p - src_p) & (RING - 1)) + own_rank

    by_axis = {
        "x": lists(my_x, my_z, src_x, src_z, own_x, own_z, (near_list, near_list_by["x"])),
        "z": lists(my_z, my_x, src_z, src_x, own_z, own_x, (near_list, near_list_by["z"])),
    }
    picks = taken(my_x, my_z, from_x, from_z) + taken(my_z, my_x, from_z, from_x)
    listed_by = {axis: jnp.concatenate([near_list, near_list_by[axis]]) for axis in ("x", "z")}

    begun = []
    for part, (axis, first, bands) in enumerate(parts):
        scalars = by_axis[axis] + (source, flat_offsets, taps, blend, listed_by[axis])
        begun.append(render(scalars, tiles, beyonds[part], first))
    arrays = []
    for part, (axis, first, bands) in enumerate(parts):
        scalars = by_axis[axis] + (source, flat_offsets, taps, blend, listed_by[axis])
        stay, up, down = render(scalars, tiles, beyonds[part], first, nears[part], nears_beyond[part], begun[part])
        came_up, came_down = hop(up, axis, 1), hop(down, axis, -1)
        packed = pack(stay, came_up, came_down)
        other = "z" if axis == "x" else "x"
        arrays += [packed[0]] + [hop(packed[lane], other, lane // 2, lane % 2) for lane in range(1, LANES)]
    shape = (per_owner, band_count, height // 2, width // 2)
    own_taken = 2 * own_src + own_rank
    return place(tuple(parts), own_taken, early, picks, arrays, shape)


def solution(mesh):
    in_specs = (
        P(("zone", "tile"), None, None, None),
        P(("zone", "tile")),
        P("zone"),
        P("zone", None),
        P("zone", None),
        P("zone"),
    )
    out_specs = P(("zone", "tile"), None, None, None)
    return jax.shard_map(local, mesh=mesh, in_specs=in_specs, out_specs=out_specs, check_vma=False)
```

```python
import functools

import jax
import jax.numpy as jnp
from jax import lax
from jax.experimental import pallas as pl
from jax.experimental.pallas import tpu as pltpu
from jax.sharding import PartitionSpec as P


EARLY = 3
PLACE_VMEM = 8 * 1024 * 1024
ABREAST = 4
STEPS = (-1, 0, 1, 2)


def passed_along(value, axis, steps):
    count = lax.axis_size(axis)
    initial, last = (max(0, -steps), min(count, count - steps))
    return lax.ppermute(value, axis, [(source, source + steps) for source in range(initial, last)])


def cubic_weight(dist):
    mag = jnp.abs(dist)
    near = (1.5 * mag - 2.5) * mag * mag + 1.0
    far = ((-0.5 * mag + 2.5) * mag - 4.0) * mag + 2.0
    return jnp.where(mag <= 1.0, near, jnp.where(mag < 2.0, far, jnp.zeros_like(mag)))


def pick_kernel(first, bands, listed_ref, tiles_ref, picked_ref, held, in_sem, out_sem):
    count = picked_ref.shape[0]
    for index in range(count):
        pltpu.make_async_copy(
            tiles_ref.at[listed_ref[index], pl.ds(first, bands)], held.at[index], in_sem.at[index]
        ).start()
    for index in range(count):
        pltpu.make_async_copy(
            tiles_ref.at[listed_ref[index], pl.ds(first, bands)], held.at[index], in_sem.at[index]
        ).wait()
        pltpu.make_async_copy(held.at[index], picked_ref.at[index], out_sem.at[index]).start()
    for index in range(count):
        pltpu.make_async_copy(held.at[index], picked_ref.at[index], out_sem.at[index]).wait()


def pick(listed, tiles, first, bands):
    shape = (listed.shape[0], bands) + tiles.shape[2:]
    return pl.pallas_call(
        functools.partial(pick_kernel, first, bands),
        out_shape=jax.ShapeDtypeStruct(shape, tiles.dtype),
        in_specs=[pl.BlockSpec(memory_space=pltpu.SMEM), pl.BlockSpec(memory_space=pl.ANY)],
        out_specs=pl.BlockSpec(memory_space=pl.ANY),
        scratch_shapes=[
            pltpu.VMEM(shape, tiles.dtype),
            pltpu.SemaphoreType.DMA((shape[0],)),
            pltpu.SemaphoreType.DMA((shape[0],)),
        ],
        name="pick",
    )(listed, tiles)


def render_kernel(
    local_count, first, bands, seams, abreast, range_ref, blocks_ref, slots_ref, source_ref, offsets_ref, taps_ref, blend_ref,
    listed_ref, tiles_ref, *refs,
):
    if seams:
        near_ref, _, out_ref, held, beside, row_lag, col_lag, done, in_sem, out_sem = refs
        load_near = pltpu.make_async_copy(near_ref, beside, in_sem.at[1])
        load_near.start()
        start, stop = range_ref[0], range_ref[1]
    else:
        out_ref, held, row_lag, col_lag, done, in_sem, out_sem = refs
        start, stop = 0, range_ref[0]
    load = pltpu.make_async_copy(tiles_ref.at[:, pl.ds(first, bands)], held, in_sem.at[0])
    load.start()
    height, width = held.shape[2], held.shape[3]
    row_lag[...] = lax.broadcasted_iota(jnp.int32, row_lag.shape, 1) - 2 * lax.broadcasted_iota(jnp.int32, row_lag.shape, 0)
    col_lag[...] = lax.broadcasted_iota(jnp.int32, col_lag.shape, 0) - 2 * lax.broadcasted_iota(jnp.int32, col_lag.shape, 1)
    load.wait()
    if seams:
        load_near.wait()

    def store(index):
        way = lax.rem(index - start, 2 * abreast)
        return pltpu.make_async_copy(done.at[way], out_ref.at[slots_ref[index]], out_sem.at[way])

    def kernel_matrix(lag_ref, block, axis):
        lag = lag_ref[...] - offsets_ref[2 * block + axis]
        kernel = jnp.zeros(lag.shape, jnp.float32)
        for place, step in enumerate(STEPS):
            kernel = jnp.where(lag == step, taps_ref[(len(STEPS) * axis + place) * source_ref.shape[0] + block], kernel)
        return kernel.astype(jnp.bfloat16)

    def render_one(index):
        block = blocks_ref[index]
        tile = lax.rem(source_ref[block], local_count)
        row_kernel = kernel_matrix(row_lag, block, 0)
        col_kernel = kernel_matrix(col_lag, block, 1)
        if seams:
            place = jnp.where(listed_ref[1] == tile, 1, 0)
            weight = blend_ref[block]
            mixed = (1.0 - weight) * held[tile].astype(jnp.float32) + weight * beside[place].astype(jnp.float32)
            mixed = mixed.astype(jnp.bfloat16)
        else:
            mixed = held[tile]
        mixed = mixed.reshape(bands * height, width)
        across = jnp.dot(mixed, col_kernel, preferred_element_type=jnp.float32).astype(jnp.bfloat16)
        beside_each = jnp.concatenate([across[b * height : (b + 1) * height] for b in range(bands)], axis=1)
        return jnp.dot(row_kernel, beside_each, preferred_element_type=jnp.float32).astype(jnp.bfloat16)

    def some(turn, carry):
        begin = start + turn * abreast
        for ahead in range(abreast):

            @pl.when(turn >= 2)
            def _():
                store(begin + ahead - 2 * abreast).wait()

        results = [render_one(jnp.minimum(begin + ahead, stop - 1)) for ahead in range(abreast)]
        for ahead in range(abreast):
            way = lax.rem(turn, 2) * abreast + ahead
            for b in range(bands):
                done[way, b] = results[ahead][:, b * (width // 2) : (b + 1) * (width // 2)]
        for ahead in range(abreast):

            @pl.when(begin + ahead < stop)
            def _():
                store(begin + ahead).start()

        return carry

    turns = lax.div(stop - start + abreast - 1, abreast)
    lax.fori_loop(0, turns, some, 0)

    def drain(index, carry):
        store(index).wait()
        return carry

    lax.fori_loop(start + jnp.maximum(turns - 2, 0) * abreast, stop, drain, 0)


def render(scalars, tiles, first, bands, slots, near=None, begun=None):
    local_count, _, height, width = tiles.shape
    block = (bands, height // 2, width // 2)
    seams = near is not None
    abreast = ABREAST
    arrays = (tiles, near, begun) if seams else (tiles,)
    flops = 12 * bands * (2 * height * width * width // 2 + height * width * height // 2)
    return pl.pallas_call(
        functools.partial(render_kernel, local_count, first, bands, seams, abreast),
        out_shape=jax.ShapeDtypeStruct((slots,) + block, jnp.bfloat16),
        in_specs=[pl.BlockSpec(memory_space=pltpu.SMEM)] * len(scalars)
        + [pl.BlockSpec(memory_space=pl.ANY)] * len(arrays),
        out_specs=pl.BlockSpec(memory_space=pl.ANY),
        scratch_shapes=[pltpu.VMEM((local_count, bands, height, width), jnp.bfloat16)]
        + ([pltpu.VMEM(near.shape, jnp.bfloat16)] if seams else [])
        + [
            pltpu.VMEM((height // 2, height), jnp.int32),
            pltpu.VMEM((width, width // 2), jnp.int32),
            pltpu.VMEM((2 * abreast,) + block, jnp.bfloat16),
            pltpu.SemaphoreType.DMA((2,)),
            pltpu.SemaphoreType.DMA((2 * abreast,)),
        ],
        input_output_aliases={len(scalars) + 2: 0} if seams else {},
        cost_estimate=pl.CostEstimate(flops=8 * flops, bytes_accessed=12 * bands * height * width // 2, transcendentals=0),
        name="seams" if seams else "render",
    )(*scalars, *arrays)


def place_kernel(taken_ref, early_ref, late_ref, out_ref, held, early_sem, late_sem, out_sem):
    count = out_ref.shape[0]
    early, late = early_ref.shape[1], late_ref.shape[1]

    def take(index):
        return pltpu.make_async_copy(early_ref.at[taken_ref[index]], held.at[index], early_sem.at[index])

    def put(index):
        return pltpu.make_async_copy(held.at[index], out_ref.at[index, pl.ds(0, early)], out_sem.at[index])

    def put_late(index):
        return pltpu.make_async_copy(
            late_ref.at[taken_ref[index]], out_ref.at[index, pl.ds(early, late)], late_sem.at[index]
        )

    for index in range(count):
        take(index).start()
    for index in range(count):
        put_late(index).start()
    for index in range(count):
        take(index).wait()
        put(index).start()
    for index in range(count):
        put(index).wait()
        put_late(index).wait()


def place(taken, early, late, count):
    shape = (count, early.shape[1] + late.shape[1]) + early.shape[2:]
    return pl.pallas_call(
        place_kernel,
        out_shape=jax.ShapeDtypeStruct(shape, jnp.bfloat16),
        in_specs=[pl.BlockSpec(memory_space=pltpu.SMEM)] + [pl.BlockSpec(memory_space=pl.ANY)] * 2,
        out_specs=pl.BlockSpec(memory_space=pl.ANY),
        scratch_shapes=[
            pltpu.VMEM((count,) + early.shape[1:], jnp.bfloat16),
            pltpu.SemaphoreType.DMA((count,)),
            pltpu.SemaphoreType.DMA((count,)),
            pltpu.SemaphoreType.DMA((count,)),
        ],
        compiler_params=pltpu.CompilerParams(vmem_limit_bytes=PLACE_VMEM),
        name="place",
    )(taken, early, late)


def swap(outgoing, capacity):
    slots = outgoing.shape[0]
    pairs = outgoing.reshape((slots // capacity, capacity) + outgoing.shape[1:])
    return lax.all_to_all(pairs, "tile", split_axis=0, concat_axis=0, tiled=True).reshape(outgoing.shape)


def local(tiles, seam_list, source, offsets, fractions, blend):
    tile_count = lax.axis_size("tile")
    myself = lax.axis_index("tile")
    zone_index = lax.axis_index("zone")
    local_count, band_count, _, _ = tiles.shape
    per_owner = source.shape[0] // tile_count
    capacity = max(2, 2 * per_owner // tile_count)
    slots = tile_count * capacity

    near_early = passed_along(pick(seam_list, tiles, 0, EARLY), "zone", 1)
    near_list = passed_along(seam_list, "zone", 1)
    near_late = passed_along(pick(seam_list, tiles, EARLY, band_count - EARLY), "zone", 1)

    tile_of = (source % local_count).reshape(tile_count, per_owner)
    src_device = (source // local_count).reshape(tile_count, per_owner)
    order_ids = jnp.arange(per_owner, dtype=jnp.int32)
    owner_ids = jnp.arange(tile_count, dtype=jnp.int32)
    mine = src_device == myself
    flagged = mine & jnp.any(tile_of[:, :, None] == near_list[None, None, :], axis=2) & (zone_index > 0)
    plain = mine & ~flagged
    earlier = order_ids[None, :] < order_ids[:, None]
    owners_ahead = owner_ids[None, :] < owner_ids[:, None]

    def place_in_line(members):
        within = jnp.sum((members[:, None, :] & earlier[None]).astype(jnp.int32), axis=2)
        each = jnp.sum(members.astype(jnp.int32), axis=1)
        ahead = jnp.sum(jnp.where(owners_ahead, each[None, :], 0), axis=1)
        return within, within + ahead[:, None], jnp.sum(each)

    plain_rank, plain_turn, plain_count = place_in_line(plain)
    seam_rank, seam_turn, seam_count = place_in_line(flagged)
    turn = jnp.where(plain, plain_turn, jnp.where(flagged, plain_count + seam_turn, -1))
    hit = turn[None] == jnp.arange(slots, dtype=jnp.int32)[:, None, None]
    block_ids = owner_ids[:, None] * per_owner + order_ids[None, :]
    slot_ids = owner_ids[:, None] * capacity + plain_rank + seam_rank
    blocks = jnp.sum(jnp.where(hit, block_ids[None], 0), axis=(1, 2))
    into = jnp.sum(jnp.where(hit, slot_ids[None], 0), axis=(1, 2))
    ranges = plain_count + jnp.arange(2, dtype=jnp.int32) * seam_count

    own = lax.dynamic_index_in_dim(src_device, myself, 0, keepdims=False)
    own_rank = jnp.sum(((own[:, None] == own[None, :]) & earlier).astype(jnp.int32), axis=1)
    taken = own * capacity + own_rank

    taps = jnp.concatenate([cubic_weight(step - fractions[:, axis]) for axis in range(2) for step in STEPS])
    scalars = (ranges, blocks, into, source, offsets.reshape(-1), taps, blend, near_list)
    outgoing = render(scalars, tiles, 0, EARLY, slots)
    outgoing = render(scalars, tiles, 0, EARLY, slots, near_early, outgoing)
    early = swap(outgoing, capacity)
    outgoing = render(scalars, tiles, EARLY, band_count - EARLY, slots)
    outgoing = render(scalars, tiles, EARLY, band_count - EARLY, slots, near_late, outgoing)
    outgoing, taken = lax.optimization_barrier((outgoing, taken))
    late = swap(outgoing, capacity)
    return place(taken, early, late, per_owner)


def solution(mesh):
    in_specs = (
        P(("zone", "tile"), None, None, None),
        P(("zone", "tile")),
        P("zone"),
        P("zone", None),
        P("zone", None),
        P("zone"),
    )
    out_specs = P(("zone", "tile"), None, None, None)
    return jax.shard_map(local, mesh=mesh, in_specs=in_specs, out_specs=out_specs, check_vma=False)
```
